32 devices in a mesh: tp: 4 (over z), cp: 8 (over y, x, core).
Axes of the slice: x: 2, y: 2, z: 4, core: 2. Of those that a mesh axis runs over, the one named last changes fastest.
Arguments:
- hidden: bfloat16 [4, 2048, 2560], P(None, 'cp')
- grad_out: bfloat16 [4, 2048, 2560], P(None, 'cp')
- w_dq: bfloat16 [2560, 768], replicated
- g_q: bfloat16 [768], replicated
- w_dkv: bfloat16 [2560, 288], replicated
- g_kv: bfloat16 [256], replicated
- w_uq: bfloat16 [768, 40, 96], P(None, 'tp')
- w_uk: bfloat16 [256, 40, 64], P(None, 'tp')
- w_uv: bfloat16 [256, 40, 64], P(None, 'tp')
- w_o: bfloat16 [40, 64, 2560], P('tp')
Outputs:
- output 1: bfloat16 [4, 2048, 2560], P(None, 'cp')
- output 2: bfloat16 [4, 2048, 2560], P(None, 'cp')
- output 3: float32 [2560, 768], replicated
- output 4: float32 [768], replicated
- output 5: float32 [2560, 288], replicated
- output 6: float32 [256], replicated
- output 7: float32 [768, 40, 96], P(None, 'tp')
- output 8: float32 [256, 40, 64], P(None, 'tp')
- output 9: float32 [256, 40, 64], P(None, 'tp')
- output 10: float32 [40, 64, 2560], P('tp')
All inputs are finite; a program needn't handle non-finite values.
Results may differ from the reference program's by a relative error of at most 0.01824.
Values are sent between devices in bfloat16 or wider.
A program may use at most 1 GiB of HBM per device.

```python
import jax
import jax.numpy as jnp
from jax import lax

D = 2560
HEADS = 40
Q_LORA = 768
KV_LORA = 256
NOPE = 64
ROPE = 32
VHEAD = 64
BATCH = 4
SEQ_DEV = 256
CP = 8
QBLK = 64
THETA = 10000

SEQ = CP * SEQ_DEV
HALF_LEN = SEQ_DEV // 2
QK_DIM = NOPE + ROPE
EPS = 1e-6
NEG_BIG = -1e30


def token_positions():
    token_idx = jnp.arange(SEQ, dtype=jnp.int32)
    cp_rank = token_idx // SEQ_DEV
    local_idx = token_idx % SEQ_DEV
    block_id = jnp.where(local_idx < HALF_LEN, cp_rank, 2 * CP - 1 - cp_rank)
    return block_id * HALF_LEN + local_idx % HALF_LEN


def rope_tables(positions):
    inv_freq = 1.0 / (THETA ** (jnp.arange(ROPE // 2, dtype=jnp.float32) * 2.0 / ROPE))
    angles = positions.astype(jnp.float32)[:, None] * inv_freq[None, :]
    return jnp.cos(angles), jnp.sin(angles)


def apply_rope(values, cos_tab, sin_tab):
    half_dim = values.shape[-1] // 2
    lead_half = values[..., :half_dim]
    tail_half = values[..., half_dim:]
    return jnp.concatenate([lead_half * cos_tab - tail_half * sin_tab, tail_half * cos_tab + lead_half * sin_tab], axis=-1)


def rms_norm(raw_vals, gain_vec):
    raw_f32 = raw_vals.astype(jnp.float32)
    inv_rms = lax.rsqrt(jnp.mean(raw_f32 * raw_f32, axis=-1, keepdims=True) + EPS)
    return (raw_f32 * inv_rms * gain_vec).astype(jnp.bfloat16)


def attention(q_nope, q_pe, k_nope, k_pe, v_heads, positions):
    kn_f32 = k_nope.astype(jnp.float32)
    kp_f32 = k_pe.astype(jnp.float32)
    v_f32 = v_heads.astype(jnp.float32)
    n_blocks = SEQ // QBLK
    qn_blocks = jnp.moveaxis(q_nope.reshape(BATCH, n_blocks, QBLK, HEADS, NOPE), 1, 0)
    qp_blocks = jnp.moveaxis(q_pe.reshape(BATCH, n_blocks, QBLK, HEADS, ROPE), 1, 0)
    pos_blocks = positions.reshape(n_blocks, QBLK)

    def one_block(block_args):
        qn_blk, qp_blk, q_pos = block_args
        scores = jnp.einsum('bqhn,bkhn->bhqk', qn_blk.astype(jnp.float32), kn_f32) + jnp.einsum('bqhr,bkr->bhqk', qp_blk.astype(jnp.float32), kp_f32)
        scores = jnp.where(positions[None, :] <= q_pos[:, None], scores * QK_DIM ** -0.5, NEG_BIG)
        weights = jax.nn.softmax(scores, axis=-1)
        return jnp.einsum('bhqk,bkhv->bqhv', weights, v_f32).astype(jnp.bfloat16)

    out_blocks = lax.map(jax.checkpoint(one_block), (qn_blocks, qp_blocks, pos_blocks))
    return jnp.moveaxis(out_blocks, 0, 1).reshape(BATCH, SEQ, HEADS, VHEAD)


def forward(hidden, w_dq, g_q, w_dkv, g_kv, w_uq, w_uk, w_uv, w_o):
    positions = token_positions()
    cos_tab, sin_tab = rope_tables(positions)
    hidden_f32 = hidden.astype(jnp.float32)
    cq_raw = jnp.einsum('btd,dq->btq', hidden_f32, w_dq).astype(jnp.bfloat16)
    kv_raw = jnp.einsum('btd,dc->btc', hidden_f32, w_dkv).astype(jnp.bfloat16)
    c_q = rms_norm(cq_raw, g_q)
    c_kv = rms_norm(kv_raw[..., :KV_LORA], g_kv)
    k_pe = apply_rope(kv_raw[..., KV_LORA:].astype(jnp.float32), cos_tab, sin_tab).astype(jnp.bfloat16)
    q_all = jnp.einsum('btq,qhe->bthe', c_q.astype(jnp.float32), w_uq).astype(jnp.bfloat16)
    q_nope = q_all[..., :NOPE]
    q_pe = apply_rope(q_all[..., NOPE:].astype(jnp.float32), cos_tab[:, None, :], sin_tab[:, None, :]).astype(jnp.bfloat16)
    k_nope = jnp.einsum('btc,chn->bthn', c_kv.astype(jnp.float32), w_uk).astype(jnp.bfloat16)
    v_heads = jnp.einsum('btc,chv->bthv', c_kv.astype(jnp.float32), w_uv).astype(jnp.bfloat16)
    o_heads = attention(q_nope, q_pe, k_nope, k_pe, v_heads, positions)
    return jnp.einsum('bthv,hvd->btd', o_heads.astype(jnp.float32), w_o).astype(jnp.bfloat16)


def setup_inputs(seed: int = 0) -> dict:
    rng_keys = jax.random.split(jax.random.key(seed), 10)

    def normal_weight(rng_key, arr_shape, fan_in):
        return (jax.random.normal(rng_key, arr_shape, jnp.float32) * fan_in ** -0.5).astype(jnp.bfloat16)

    return {
        'hidden': jax.random.normal(rng_keys[0], (BATCH, SEQ, D), jnp.float32).astype(jnp.bfloat16),
        'grad_out': jax.random.normal(rng_keys[1], (BATCH, SEQ, D), jnp.float32).astype(jnp.bfloat16),
        'w_dq': normal_weight(rng_keys[2], (D, Q_LORA), D),
        'g_q': jax.random.uniform(rng_keys[3], (Q_LORA,), jnp.float32, 0.5, 1.5).astype(jnp.bfloat16),
        'w_dkv': normal_weight(rng_keys[4], (D, KV_LORA + ROPE), D),
        'g_kv': jax.random.uniform(rng_keys[5], (KV_LORA,), jnp.float32, 0.5, 1.5).astype(jnp.bfloat16),
        'w_uq': normal_weight(rng_keys[6], (Q_LORA, HEADS, QK_DIM), Q_LORA),
        'w_uk': normal_weight(rng_keys[7], (KV_LORA, HEADS, NOPE), KV_LORA),
        'w_uv': normal_weight(rng_keys[8], (KV_LORA, HEADS, VHEAD), KV_LORA),
        'w_o': normal_weight(rng_keys[9], (HEADS, VHEAD, D), HEADS * VHEAD),
    }


def reference(hidden, grad_out, w_dq, g_q, w_dkv, g_kv, w_uq, w_uk, w_uv, w_o):
    attn_out, pullback = jax.vjp(forward, hidden, w_dq.astype(jnp.float32), g_q.astype(jnp.float32), w_dkv.astype(jnp.float32), g_kv.astype(jnp.float32), w_uq.astype(jnp.float32), w_uk.astype(jnp.float32), w_uv.astype(jnp.float32), w_o.astype(jnp.float32))
    all_grads = pullback(grad_out)
    return (attn_out, all_grads[0], all_grads[1], all_grads[2], all_grads[3], all_grads[4], all_grads[5], all_grads[6], all_grads[7], all_grads[8])
```

```python
import functools
import math

import jax
import jax.numpy as jnp
from jax import lax
from jax.experimental import pallas as pl
from jax.experimental.pallas import tpu as pltpu
from jax.sharding import PartitionSpec as P

EPS = 1e-6
THETA = 10000.0
NEG_BIG = -1e30
BF = jnp.bfloat16
F32 = jnp.float32
NT = (((1,), (1,)), ((), ()))
TN = (((0,), (0,)), ((), ()))
NN = (((1,), (0,)), ((), ()))
HB, QB, CH, SEQ = 128, 256, 512, 2048
HD, KD, LAT, QL = 64, 160, 288, 768
NBLK, NCP, NTP, NPAIR = 16, 8, 4, 5
TOK, DM, HV, QW, ALL = 1024, 2560, 640, 1280, 1056
RH = 16


def dot(a, b, dims):
    return lax.dot_general(a, b, dims, preferred_element_type=F32)


def owner(blk):
    if blk < NCP:
        return blk, slice(0, HB)
    return NBLK - 1 - blk, slice(HB, QB)


def attn_kernel(r_ref, q_ref, do_ref, wk_ref, wv_ref, cos_ref, sin_ref, *rest):
    kv_ref, o_ref, dq_ref, dw_ref, dkv_ref, ckv, ckvt, kcat, vv, s_scr, dp_scr, dk_acc, dv_acc, dckv, dkpe, qbd, dobd = rest
    b = pl.program_id(0)
    p = pl.program_id(1)
    n_pair = pl.num_programs(1)
    r = r_ref[0]
    scale = 96.0 ** -0.5
    c2 = scale * math.log2(math.e)

    @pl.when(p == 0)
    def _():
        for blk in range(NBLK):
            rows = slice(blk * HB, (blk + 1) * HB)
            dev, part = owner(blk)
            ckv[rows, :] = kv_ref[dev, 0, part, 0:QB]
            kcat[rows, HB:KD] = kv_ref[dev, 0, part, QB:LAT]
        for i in range(4):
            ckvt[:, i * CH:(i + 1) * CH] = ckv[i * CH:(i + 1) * CH, :].T
        dckv[...] = jnp.zeros_like(dckv)
        dkpe[...] = jnp.zeros_like(dkpe)

    wkv = jnp.concatenate([wk_ref[...], wv_ref[...]], axis=1)
    for i in range(4):
        rows = slice(i * CH, (i + 1) * CH)
        kv = dot(ckv[rows, :], wkv, NN).astype(BF)
        kcat[rows, 0:HB] = kv[:, 0:HB]
        vv[rows, :] = kv[:, HB:QB]

    cos_t = cos_ref[...]
    sin_t = sin_ref[...]
    lane = lax.broadcasted_iota(jnp.int32, (HB, HB), 1)
    zero = jnp.zeros((HB, HB), BF)
    qpt = q_ref[0, :, HB:QB].astype(F32).T
    roped = []
    for h in range(2):
        u1 = qpt[h * 32:h * 32 + 16, :]
        u2 = qpt[h * 32 + 16:h * 32 + 32, :]
        roped.append(u1 * cos_t - u2 * sin_t)
        roped.append(u2 * cos_t + u1 * sin_t)
    qpe = jnp.concatenate(roped + [jnp.zeros((HD, QB), F32)], axis=0).T.astype(BF)
    for s in range(2):
        rows = slice(s * HB, (s + 1) * HB)
        qn = q_ref[0, rows, 0:HB]
        gg = do_ref[0, rows, :]
        qbd[s, 0:HB, 0:HB] = jnp.where(lane < HD, qn, zero)
        qbd[s, HB:QB, 0:HB] = jnp.where(lane < HD, zero, qn)
        qbd[s, 0:HB, HB:KD] = qpe[rows, 0:32]
        qbd[s, HB:QB, HB:KD] = qpe[rows, 32:64]
        dobd[s, 0:HB, :] = jnp.where(lane < HD, gg, zero)
        dobd[s, HB:QB, :] = jnp.where(lane < HD, zero, gg)

    low = r < 4
    sel3 = jnp.where(low, 1, 0)
    chunks = [(1, 0), (1, 1), (1, 2), (sel3, jnp.where(low, 3, 0)), (0, jnp.where(low, 0, 1))]

    def keys(c):
        kc = chunks[c][1]
        if isinstance(kc, int):
            return slice(kc * CH, (kc + 1) * CH)
        return pl.ds(pl.multiple_of(kc * CH, CH), CH)

    diff = (lax.broadcasted_iota(jnp.int32, (CH, QB), 0)
            - lax.rem(lax.broadcasted_iota(jnp.int32, (CH, QB), 1), HB))
    maxes = []
    for c in range(5):
        sel, kc = chunks[c]
        s = dot(kcat[keys(c), :], qbd[sel], NT)
        if c >= 2:
            blk = jnp.where(sel == 1, 15 - r, r)
            s = jnp.where(diff <= blk * HB - kc * CH, s, NEG_BIG)
        s_scr[c] = s
        maxes.append(jnp.max(s, axis=0, keepdims=True))

    def join(vals, op, ident):
        ident = jnp.full_like(vals[3], ident)
        top = op(op(op(vals[0], vals[1]), vals[2]), jnp.where(low, vals[3], ident))
        bot = op(vals[4], jnp.where(low, ident, vals[3]))
        return [top, top, top, jnp.where(low, top, bot), bot]

    m = join(maxes, jnp.maximum, NEG_BIG)
    sums, dots = [], []
    for c in range(5):
        sel, kc = chunks[c]
        e = jnp.exp2((s_scr[c] - m[c]) * c2)
        s_scr[c] = e
        sums.append(jnp.sum(e, axis=0, keepdims=True))
        dp = dot(vv[keys(c), :], dobd[sel], NT)
        dp_scr[c] = dp
        dots.append(jnp.sum(e * dp, axis=0, keepdims=True))
    total = join(sums, jnp.add, 0.0)
    inv = [1.0 / t for t in total]
    dsum = join(dots, jnp.add, 0.0)
    delta = [d * i for d, i in zip(dsum, inv)]
    ots, dqts = [], []
    dk_acc[3 * CH:SEQ, :] = jnp.zeros((CH, KD), F32)
    dv_acc[3 * CH:SEQ, :] = jnp.zeros((CH, HB), F32)
    for c in range(5):
        sel, kc = chunks[c]
        pr = s_scr[c] * inv[c]
        pb = pr.astype(BF)
        ds = (pr * (dp_scr[c] - delta[c])).astype(BF)
        ots.append(dot(vv[keys(c), :], pb, TN))
        dqts.append(dot(kcat[keys(c), :], ds, TN))
        dv = dot(pb, dobd[sel], NN)
        dk = dot(ds, qbd[sel], NN)
        if c < 3:
            dk_acc[keys(c), :] = dk
            dv_acc[keys(c), :] = dv
        else:
            dk_acc[keys(c), :] += dk
            dv_acc[keys(c), :] += dv
    ot = join(ots, jnp.add, 0.0)
    dqt = join(dqts, jnp.add, 0.0)
    for s in range(2):
        rows = slice(s * HB, (s + 1) * HB)
        a = ot[0 if s == 1 else 4]
        o_ref[0, rows, :] = jnp.concatenate([a[0:HD, 0:HB], a[HD:HB, HB:QB]], axis=0).T.astype(BF)
        g = dqt[0 if s == 1 else 4] * scale
        dq_ref[0, rows, 0:HB] = jnp.concatenate([g[0:HD, 0:HB], g[HD:HB, HB:QB]], axis=0).T.astype(BF)
        pe = []
        for h in range(2):
            g1 = g[128:144, h * HB:(h + 1) * HB]
            g2 = g[144:160, h * HB:(h + 1) * HB]
            ct = cos_t[:, rows]
            st = sin_t[:, rows]
            pe.append(g1 * ct + g2 * st)
            pe.append(g2 * ct - g1 * st)
        dq_ref[0, rows, HB:QB] = jnp.concatenate(pe + [jnp.zeros((HD, HB), F32)], axis=0).T.astype(BF)

    dwt = jnp.zeros((QB, QB), F32)
    for i in range(4):
        rows = slice(i * CH, (i + 1) * CH)
        dkv = jnp.concatenate([(dk_acc[rows, 0:HB] * scale).astype(BF), dv_acc[rows, :].astype(BF)], axis=1)
        dkpe[rows, :] += dk_acc[rows, HB:KD] * scale
        dckv[rows, :] += dot(dkv, wkv, NT)
        dwt = dwt + dot(ckvt[:, rows], dkv, NN)

    @pl.when(b == 0)
    def _():
        dw_ref[p] = dwt

    @pl.when(b > 0)
    def _():
        dw_ref[p] += dwt

    @pl.when(p == n_pair - 1)
    def _():
        for blk in range(NBLK):
            rows = slice(blk * HB, (blk + 1) * HB)
            dev, part = owner(blk)
            dkv_ref[dev, 0, part, 0:QB] = dckv[rows, :].astype(BF)
            dkv_ref[dev, 0, part, QB:LAT] = dkpe[rows, :].astype(BF)


def attention(rank, q, do, wk, wv, cos_t, sin_t, kv, b0, nb):
    pair_blk = lambda w: pl.BlockSpec((1, QB, w), lambda b, p, *_: (b0 + b, 0, p))
    out_blk = lambda w: pl.BlockSpec((1, QB, w), lambda b, p, *_: (b, 0, p))
    w_blk = pl.BlockSpec((QB, HB), lambda b, p, *_: (0, p))
    full = pl.BlockSpec((16, QB), lambda b, p, *_: (0, 0))
    kv_blk = pl.BlockSpec((NCP, 1, QB, LAT), lambda b, p, *_: (0, b0 + b, 0, 0))
    dkv_blk = pl.BlockSpec((NCP, 1, QB, LAT), lambda b, p, *_: (0, b, 0, 0))
    grid_spec = pltpu.PrefetchScalarGridSpec(
        num_scalar_prefetch=1,
        grid=(nb, NPAIR),
        in_specs=[pair_blk(QB), pair_blk(HB), w_blk, w_blk, full, full, kv_blk],
        out_specs=[out_blk(HB), out_blk(QB), pl.BlockSpec((NPAIR, QB, QB), lambda b, p, *_: (0, 0, 0)), dkv_blk],
        scratch_shapes=[
            pltpu.VMEM((SEQ, QB), BF), pltpu.VMEM((QB, SEQ), BF), pltpu.VMEM((SEQ, KD), BF), pltpu.VMEM((SEQ, HB), BF),
            pltpu.VMEM((5, CH, QB), F32), pltpu.VMEM((5, CH, QB), F32),
            pltpu.VMEM((SEQ, KD), F32), pltpu.VMEM((SEQ, HB), F32),
            pltpu.VMEM((SEQ, QB), F32), pltpu.VMEM((SEQ, 32), F32),
            pltpu.VMEM((2, QB, KD), BF), pltpu.VMEM((2, QB, HB), BF),
        ])
    return pl.pallas_call(
        attn_kernel,
        grid_spec=grid_spec,
        out_shape=[jax.ShapeDtypeStruct((nb, QB, HV), BF), jax.ShapeDtypeStruct((nb, QB, QW), BF), jax.ShapeDtypeStruct((NPAIR, QB, QB), F32),
                   jax.ShapeDtypeStruct((NCP, nb, QB, LAT), BF)],
        compiler_params=pltpu.CompilerParams(vmem_limit_bytes=50 * 1024 * 1024),
        cost_estimate=pl.CostEstimate(flops=nb * 20_000_000_000, bytes_accessed=nb * 8_000_000, transcendentals=0),
        name="attn",
    )(rank, q, do, wk, wv, cos_t, sin_t, kv)


def plane_kernel(n_arr, reduce, gather, n_z, *refs):
    ins, refs = refs[:n_arr], refs[n_arr:]
    outs, refs = refs[:n_arr], refs[n_arr:]
    r = lax.axis_index('cp')
    z = lax.axis_index('tp')
    send, recv, scratch = refs[0], refs[1], refs[2:]
    peers = {1: {'cp': r ^ 1}, 2: {'cp': r ^ 2}, 4: {'cp': r ^ 4}}
    barrier = pltpu.get_barrier_semaphore()
    targets = list(peers.values()) + [{'tp': lax.rem(z + d, NTP)} for d in range(1, n_z)]
    for t in targets:
        pl.semaphore_signal(barrier, inc=1, device_id=t, device_id_type=pl.DeviceIdType.MESH)
    pl.semaphore_wait(barrier, len(targets))
    count = [0]
    started = []

    def copy(src, dst, target):
        k = count[0]
        count[0] += 1
        c = pltpu.make_async_remote_copy(src_ref=src, dst_ref=dst, send_sem=send.at[k], recv_sem=recv.at[k],
                                         device_id=target, device_id_type=pl.DeviceIdType.MESH)
        c.start()
        started.append(c)
        return c

    work = []
    for i in range(n_arr):
        w = {'in': ins[i], 'out': outs[i]}
        if reduce:
            w['rc'], w['sb'], w['rd'], w['rx'], w['ry'] = scratch[:5]
            scratch = scratch[5:]
            rows = w['rd'].shape[0]
        else:
            rows = ins[i].shape[0]
        if gather:
            w['g'] = scratch[0]
            scratch = scratch[1:]
        w['a'] = slice(0, (rows // 2 + RH - 1) // RH * RH)
        w['b'] = slice(w['a'].stop, rows)
        work.append(w)
    if reduce:
        for w in work:
            w['c'] = [None] * 4
        for k in (3, 1, 2, 0):
            for w in work:
                w['c'][k] = copy(w['in'].at[r ^ (2 * k + 1)], w['rc'].at[k], peers[1])

        def local(w, k):
            w['c'][k].wait_recv()
            return w['in'][r ^ (2 * k)].astype(F32) + w['rc'][k].astype(F32)

        for w in work:
            w['sb'][3] = local(w, 3).astype(BF)
            w['da'] = copy(w['sb'].at[3, w['a']], w['rd'].at[w['a']], peers[2])
            w['db'] = copy(w['sb'].at[3, w['b']], w['rd'].at[w['b']], peers[4])
        for w in work:
            w['sb'][1] = local(w, 1).astype(BF)
            w['xa'] = copy(w['sb'].at[1, w['a']], w['rx'].at[w['a']], peers[2])
            w['sb'][2] = local(w, 2).astype(BF)
            w['yb'] = copy(w['sb'].at[2, w['b']], w['ry'].at[w['b']], peers[4])
        for w in work:
            w['da'].wait_recv()
            w['sb'][2, w['a']] = (w['sb'][2, w['a']].astype(F32) + w['rd'][w['a']].astype(F32)).astype(BF)
            w['ya'] = copy(w['sb'].at[2, w['a']], w['ry'].at[w['a']], peers[4])
            w['db'].wait_recv()
            w['sb'][1, w['b']] = (w['sb'][1, w['b']].astype(F32) + w['rd'][w['b']].astype(F32)).astype(BF)
            w['xb'] = copy(w['sb'].at[1, w['b']], w['rx'].at[w['b']], peers[2])
        for w in work:
            base = local(w, 0)
            for name in ('xa', 'yb', 'ya', 'xb'):
                w[name].wait_recv()
            total = base + w['rx'][...].astype(F32) + w['ry'][...].astype(F32)
            if gather:
                w['g'][z * NCP * (n_z > 1) + r] = total.astype(BF)
            else:
                w['out'][...] = total
    elif gather:
        for w in work:
            w['g'][r] = w['in'][...]
    if gather:
        def fan(w, zz):
            own = w['g'].at[zz + r]
            return {'zz': zz, 2: copy(own, own, peers[2]), 4: copy(own, own, peers[4]), 1: copy(own, own, peers[1])}

        flows = []
        z_copies = []
        for w in work:
            if n_z > 1:
                own = w['g'].at[z * NCP + r]
                z_copies.append([copy(own, own, {'tp': lax.rem(z + d, NTP)}) for d in range(1, n_z)])
            flows.append([fan(w, z * NCP if n_z > 1 else 0)])
        for d in range(n_z):
            for i, w in enumerate(work):
                f = flows[i][d]
                gx, gy = w['g'].at[f['zz'] + (r ^ 2)], w['g'].at[f['zz'] + (r ^ 4)]
                f[2].wait_recv()
                f['dy'] = copy(gx.at[w['b']], gx.at[w['b']], peers[4])
                f['cx'] = copy(gx, gx, peers[1])
                f[4].wait_recv()
                f['dx'] = copy(gy.at[w['a']], gy.at[w['a']], peers[2])
                f['cy'] = copy(gy, gy, peers[1])
                if d + 1 < n_z:
                    z_copies[i][d].wait_recv()
                    flows[i].append(fan(w, lax.rem(z + NTP - (d + 1), NTP) * NCP))
        for d in range(n_z):
            for i, w in enumerate(work):
                f = flows[i][d]
                f['dy'].wait_recv()
                f['dx'].wait_recv()
                gd = w['g'].at[f['zz'] + (r ^ 6)]
                f['cd'] = copy(gd, gd, peers[1])
        for d in range(n_z):
            for i, w in enumerate(work):
                f = flows[i][d]
                for name in (1, 'cx', 'cy', 'cd'):
                    f[name].wait_recv()
        for w in work:
            w['out'][...] = w['g'][...]
    for c in started:
        c.wait_send()


def plane(arrs, cid, reduce, gather, n_z=1):
    scratch, shapes = [], []
    n_copy = 0
    for v in arrs:
        n, m = v.shape[-2:]
        if reduce:
            scratch += [pltpu.VMEM((4, n, m), BF), pltpu.VMEM((4, n, m), BF)] + [pltpu.VMEM((n, m), BF)] * 3
            n_copy += 10
        if gather:
            scratch.append(pltpu.VMEM((NCP * n_z, n, m), BF))
            shapes.append(jax.ShapeDtypeStruct((NCP * n_z, n, m), BF))
            n_copy += 8 * n_z + n_z - 1
        else:
            shapes.append(jax.ShapeDtypeStruct((n, m), F32))
    vmem = pl.BlockSpec(memory_space=pltpu.VMEM)
    return pl.pallas_call(
        functools.partial(plane_kernel, len(arrs), reduce, gather, n_z),
        out_shape=shapes,
        in_specs=[vmem] * len(arrs),
        out_specs=[vmem] * len(arrs),
        scratch_shapes=[pltpu.SemaphoreType.DMA((n_copy,)), pltpu.SemaphoreType.DMA((n_copy,))] + scratch,
        compiler_params=pltpu.CompilerParams(collective_id=cid, has_side_effects=True, vmem_limit_bytes=60 * TOK * TOK),
        cost_estimate=pl.CostEstimate(flops=30_000_000_000, bytes_accessed=10_000_000, transcendentals=0),
        name="plane",
    )(*arrs)


def zshift(v, d):
    return lax.ppermute(v, 'tp', [(i, (i + d) % NTP) for i in range(NTP)])


def zgather(v, z):
    rel = [v] + [zshift(v, d) for d in range(1, NTP)]
    return [lax.select_n((z - j) % NTP, *rel) for j in range(NTP)]


def norm_f32(raw_vals, gain_vec):
    inv_rms = lax.rsqrt(jnp.mean(raw_vals * raw_vals, axis=-1, keepdims=True) + EPS)
    return raw_vals * inv_rms * gain_vec


def solution(mesh):
    def per_device(hidden, grad_out, w_dq, g_q, w_dkv, g_kv, w_uq, w_uk, w_uv, w_o):
        rank = lax.axis_index('cp')
        z = lax.axis_index('tp')
        x2 = hidden.reshape(TOK, DM)
        dy2 = grad_out.reshape(TOK, DM)
        half = 16
        inv_freq = 1.0 / (THETA ** (jnp.arange(half, dtype=F32) * 2.0 / 32))
        idx = jnp.arange(QB, dtype=jnp.int32)
        positions = jnp.where(idx < HB, rank, NBLK - 1 - rank) * HB + idx % HB
        angles = positions.astype(F32)[:, None] * inv_freq[None, :]
        cos_tab, sin_tab = jnp.cos(angles), jnp.sin(angles)
        cos_t, sin_t = cos_tab.T, sin_tab.T
        gq = g_q.astype(F32)
        gkv = g_kv.astype(F32)

        kv_raw = dot(x2, w_dkv, NN).astype(BF)
        ckv_f32 = kv_raw[:, :QB].astype(F32)
        c_kv = norm_f32(ckv_f32, gkv).astype(BF)
        pe = kv_raw[:, QB:].astype(F32).reshape(4, QB, 32)
        pe1, pe2 = pe[..., :half], pe[..., half:]
        k_pe = jnp.concatenate([pe1 * cos_tab - pe2 * sin_tab, pe2 * cos_tab + pe1 * sin_tab], axis=-1).astype(BF)
        kv, = plane([jnp.concatenate([c_kv, k_pe.reshape(TOK, 32)], axis=-1)], 0, False, True)
        kv = kv.reshape(NCP, 4, QB, LAT)

        wo2 = w_o.reshape(HV, DM)
        wo_slice, kv = lax.optimization_barrier((lax.dynamic_slice_in_dim(wo2, rank * 80, 80, 0), kv))
        wo_all = lax.all_gather(wo_slice, ('tp', 'cp'), axis=0, tiled=True)

        cq_raw = dot(x2, w_dq, NN).astype(BF)
        cq_f32 = cq_raw.astype(F32)
        c_q = norm_f32(cq_f32, gq).astype(BF)
        w_q = jnp.concatenate([w_uq[:, :, :HD].reshape(QL, NPAIR, HB), w_uq[:, :, HD:].reshape(QL, NPAIR, HD), jnp.zeros((QL, NPAIR, HD), BF)], axis=2).reshape(QL, QW)
        q = dot(c_q, w_q, NN).astype(BF).reshape(4, QB, QW)
        do = dot(dy2, wo2, NT).astype(BF).reshape(4, QB, HV)
        wk = w_uk.reshape(QB, HV)
        wv = w_uv.reshape(QB, HV)

        n_split = 2
        nb = 4 // n_split
        runs = [attention(rank.reshape(1), q, do, wk, wv, cos_t, sin_t, kv, i * nb, nb) for i in range(n_split)]
        o_all = [zgather(run[0], z) for run in runs]
        o_all = jnp.concatenate([jnp.concatenate(parts, axis=2) for parts in o_all], axis=0).reshape(TOK, NTP * HV)
        attn_out = dot(o_all, wo_all, NN).astype(BF).reshape(4, QB, DM)
        o = jnp.concatenate([run[0] for run in runs], axis=0).reshape(TOK, HV)
        dq = jnp.concatenate([run[1] for run in runs], axis=0).reshape(TOK, QW)
        dwkv = sum(run[2] for run in runs)
        dkv = jnp.concatenate([run[3] for run in runs], axis=1).reshape(NCP, TOK, LAT)

        dckv, = plane([dkv], 1, True, False)
        lat_q = dot(dq, w_q, NT)
        lat = jnp.concatenate([lat_q, dckv], axis=-1).reshape(4, QB, ALL)
        lat_bf = lat.astype(BF)
        own = lax.dynamic_index_in_dim(lat, z, 0, keepdims=False)
        for d in range(1, NTP):
            mine = lax.dynamic_index_in_dim(lat_bf, (z + d) % NTP, 0, keepdims=False)
            own = own + zshift(mine, d).astype(F32)

        cq_own = lax.dynamic_slice_in_dim(cq_f32, z * QB, QB, 0)
        ckv_own = lax.dynamic_slice_in_dim(ckv_f32, z * QB, QB, 0)
        g_cq, grad_g_q = jax.vjp(norm_f32, cq_own, gq)[1](own[:, :QL])
        g_ckv, grad_g_kv = jax.vjp(norm_f32, ckv_own, gkv)[1](own[:, QL:TOK])
        p1, p2 = own[:, TOK:TOK + half], own[:, TOK + half:]
        raw = jnp.concatenate([g_cq, g_ckv, p1 * cos_tab + p2 * sin_tab, p2 * cos_tab - p1 * sin_tab], axis=-1).astype(BF)
        raw_all = jnp.concatenate(zgather(raw, z), axis=0)

        x_slice = lax.dynamic_slice_in_dim(x2, z * HV, HV, 1)
        dwd = dot(x_slice, raw_all, TN).astype(BF).reshape(NCP, 80, ALL)
        dwd, = plane([dwd], 2, True, True, NTP)
        dwd = dwd.reshape(DM, ALL).astype(F32)
        w_d = jnp.concatenate([w_dq, w_dkv], axis=1)
        grad_hidden = dot(raw_all, w_d, NT).astype(BF).reshape(4, QB, DM)

        dwq = dot(c_q, dq, TN).astype(BF).reshape(NCP, 96, QW)
        dwkv = dwkv.transpose(1, 0, 2).reshape(NCP, 32, QW).astype(BF)
        dwo = dot(o, dy2, TN).astype(BF).reshape(NCP, 80, DM)
        dwq, dwkv, dwo = plane([dwq, dwkv, dwo], 3, True, True)
        grad_g_q, grad_g_kv = lax.psum((grad_g_q, grad_g_kv), ('tp', 'cp'))
        dwq = dwq.reshape(QL, NPAIR, QB).astype(F32)
        grad_uq = jnp.concatenate([dwq[:, :, :HB].reshape(QL, 10, HD), dwq[:, :, HB:HB + HD].reshape(QL, 10, 32)], axis=-1)
        dwkv = dwkv.reshape(QB, NPAIR, QB).astype(F32)
        grad_uk = dwkv[:, :, :HB].reshape(QB, 10, HD)
        grad_uv = dwkv[:, :, HB:].reshape(QB, 10, HD)
        return (attn_out, grad_hidden, dwd[:, :QL], grad_g_q, dwd[:, QL:], grad_g_kv, grad_uq, grad_uk, grad_uv, dwo.reshape(10, HD, DM).astype(F32))

    seq_spec = P(None, 'cp', None)
    full_spec = P()
    head_spec = P(None, 'tp', None)
    out_head_spec = P('tp', None, None)
    all_specs = (seq_spec, seq_spec, full_spec, full_spec, full_spec, full_spec, head_spec, head_spec, head_spec, out_head_spec)
    return jax.shard_map(per_device, mesh=mesh, in_specs=all_specs, out_specs=all_specs, check_vma=False)
```

```python
import functools
import math

import jax
import jax.numpy as jnp
from jax import lax
from jax.experimental import pallas as pl
from jax.experimental.pallas import tpu as pltpu
from jax.sharding import PartitionSpec as P


EPS = 1e-6
THETA = 10000.0
NEG_BIG = -1e30
BF = jnp.bfloat16
F32 = jnp.float32
NT = (((1,), (1,)), ((), ()))
TN = (((0,), (0,)), ((), ()))
NN = (((1,), (0,)), ((), ()))
HB, QB, CH, SEQ = 128, 256, 512, 2048
HD, KD, RD, QL = 64, 160, 32, 768
NBLK, NCP, NTP, NPAIR = 16, 8, 4, 5
TOK, DM, HV, QW, ALL, DWW = 1024, 2560, 640, 1280, 1056, 1152
RH = 16


def dot(a, b, dims):
    return lax.dot_general(a, b, dims, preferred_element_type=F32)


def owner(blk):
    if blk < NCP:
        return blk, slice(0, HB)
    return NBLK - 1 - blk, slice(HB, QB)


def attn_kernel(b0, n_batch, r_ref, q_ref, do_ref, wk_ref, wv_ref, cos_ref, sin_ref, *rest):
    kv_ref, kpe_ref = rest[:2]
    rest = rest[2 if b0 == 0 else 4:]
    o_ref, dq_ref, dw_ref, dkv_ref, dkpe_ref, ckv, ckvt, kcat, vv, s_scr, dp_scr, dk_acc, dv_acc, dckv, dkpe, qbd, dobd = rest
    b = pl.program_id(0)
    p = pl.program_id(1)
    n_pair = pl.num_programs(1)
    r = r_ref[0]
    scale = 96.0 ** -0.5
    c2 = scale * math.log2(math.e)

    @pl.when(p == 0)
    def _():
        for blk in range(NBLK):
            rows = slice(blk * HB, (blk + 1) * HB)
            dev, part = owner(blk)
            ckv[rows, :] = kv_ref[dev, 0, part, :]
            for i in range(n_batch):
                @pl.when(b == i)
                def _():
                    kcat[rows, HB:KD] = kpe_ref[dev, part, (b0 + i) * RD:(b0 + i + 1) * RD]
        for i in range(4):
            ckvt[:, i * CH:(i + 1) * CH] = ckv[i * CH:(i + 1) * CH, :].T
        dckv[...] = jnp.zeros_like(dckv)
        dkpe[...] = jnp.zeros_like(dkpe)

    wkv = jnp.concatenate([wk_ref[...], wv_ref[...]], axis=0)
    for i in range(4):
        rows = slice(i * CH, (i + 1) * CH)
        kv = dot(ckv[rows, :], wkv, NT).astype(BF)
        kcat[rows, 0:HB] = kv[:, 0:HB]
        vv[rows, :] = kv[:, HB:QB]

    cos_t = cos_ref[...]
    sin_t = sin_ref[...]
    lane = lax.broadcasted_iota(jnp.int32, (HB, HB), 1)
    zero = jnp.zeros((HB, HB), BF)
    qpt = q_ref[0, :, HB:QB].astype(F32).T
    roped = []
    for h in range(2):
        u1 = qpt[h * 32:h * 32 + 16, :]
        u2 = qpt[h * 32 + 16:h * 32 + 32, :]
        roped.append(u1 * cos_t - u2 * sin_t)
        roped.append(u2 * cos_t + u1 * sin_t)
    qpe = jnp.concatenate(roped + [jnp.zeros((HD, QB), F32)], axis=0).T.astype(BF)
    for s in range(2):
        rows = slice(s * HB, (s + 1) * HB)
        qn = q_ref[0, rows, 0:HB]
        gg = do_ref[0, rows, :]
        qbd[s, 0:HB, 0:HB] = jnp.where(lane < HD, qn, zero)
        qbd[s, HB:QB, 0:HB] = jnp.where(lane < HD, zero, qn)
        qbd[s, 0:HB, HB:KD] = qpe[rows, 0:32]
        qbd[s, HB:QB, HB:KD] = qpe[rows, 32:64]
        dobd[s, 0:HB, :] = jnp.where(lane < HD, gg, zero)
        dobd[s, HB:QB, :] = jnp.where(lane < HD, zero, gg)

    low = r < 4
    sel3 = jnp.where(low, 1, 0)
    chunks = [(1, 0), (1, 1), (1, 2), (sel3, jnp.where(low, 3, 0)), (0, jnp.where(low, 0, 1))]

    def keys(c):
        kc = chunks[c][1]
        if isinstance(kc, int):
            return slice(kc * CH, (kc + 1) * CH)
        return pl.ds(pl.multiple_of(kc * CH, CH), CH)

    diff = (lax.broadcasted_iota(jnp.int32, (CH, QB), 0)
            - lax.rem(lax.broadcasted_iota(jnp.int32, (CH, QB), 1), HB))
    maxes = []
    for c in range(5):
        sel, kc = chunks[c]
        s = dot(kcat[keys(c), :], qbd[sel], NT)
        if c >= 2:
            blk = jnp.where(sel == 1, 15 - r, r)
            s = jnp.where(diff <= blk * HB - kc * CH, s, NEG_BIG)
        s_scr[c] = s
        maxes.append(jnp.max(s, axis=0, keepdims=True))

    def join(vals, op, ident):
        ident = jnp.full_like(vals[3], ident)
        top = op(op(op(vals[0], vals[1]), vals[2]), jnp.where(low, vals[3], ident))
        bot = op(vals[4], jnp.where(low, ident, vals[3]))
        return [top, top, top, jnp.where(low, top, bot), bot]

    m = join(maxes, jnp.maximum, NEG_BIG)
    sums, dots = [], []
    for c in range(5):
        sel, kc = chunks[c]
        e = jnp.exp2((s_scr[c] - m[c]) * c2)
        s_scr[c] = e
        sums.append(jnp.sum(e, axis=0, keepdims=True))
        dp = dot(vv[keys(c), :], dobd[sel], NT)
        dp_scr[c] = dp
        dots.append(jnp.sum(e * dp, axis=0, keepdims=True))
    total = join(sums, jnp.add, 0.0)
    inv = [1.0 / t for t in total]
    dsum = join(dots, jnp.add, 0.0)
    delta = [d * i for d, i in zip(dsum, inv)]
    ots, dqts = [], []
    dk_acc[3 * CH:SEQ, :] = jnp.zeros((CH, KD), F32)
    dv_acc[3 * CH:SEQ, :] = jnp.zeros((CH, HB), F32)
    for c in range(5):
        sel, kc = chunks[c]
        pr = s_scr[c] * inv[c]
        pb = pr.astype(BF)
        ds = (pr * (dp_scr[c] - delta[c])).astype(BF)
        ots.append(dot(vv[keys(c), :], pb, TN))
        dqts.append(dot(kcat[keys(c), :], ds, TN))
        dv = dot(pb, dobd[sel], NN)
        dk = dot(ds, qbd[sel], NN)
        if c < 3:
            dk_acc[keys(c), :] = dk
            dv_acc[keys(c), :] = dv
        else:
            dk_acc[keys(c), :] += dk
            dv_acc[keys(c), :] += dv
    ot = join(ots, jnp.add, 0.0)
    dqt = join(dqts, jnp.add, 0.0)
    for s in range(2):
        rows = slice(s * HB, (s + 1) * HB)
        a = ot[0 if s == 1 else 4]
        o_ref[0, rows, :] = jnp.concatenate([a[0:HD, 0:HB], a[HD:HB, HB:QB]], axis=0).T.astype(BF)
        g = dqt[0 if s == 1 else 4] * scale
        dq_ref[0, rows, 0:HB] = jnp.concatenate([g[0:HD, 0:HB], g[HD:HB, HB:QB]], axis=0).T.astype(BF)
        pe = []
        for h in range(2):
            g1 = g[128:144, h * HB:(h + 1) * HB]
            g2 = g[144:160, h * HB:(h + 1) * HB]
            ct = cos_t[:, rows]
            st = sin_t[:, rows]
            pe.append(g1 * ct + g2 * st)
            pe.append(g2 * ct - g1 * st)
        dq_ref[0, rows, HB:QB] = jnp.concatenate(pe + [jnp.zeros((HD, HB), F32)], axis=0).T.astype(BF)

    dwt = jnp.zeros((QB, QB), F32)
    for i in range(4):
        rows = slice(i * CH, (i + 1) * CH)
        dkv = jnp.concatenate([(dk_acc[rows, 0:HB] * scale).astype(BF), dv_acc[rows, :].astype(BF)], axis=1)
        dkpe[rows, :] += dk_acc[rows, HB:KD] * scale
        dckv[rows, :] += dot(dkv, wkv, NN)
        dwt = dwt + dot(ckvt[:, rows], dkv, NN)
    dwt = dwt.T

    @pl.when(b == 0)
    def _():
        dw_ref[p] = dwt

    @pl.when(b > 0)
    def _():
        dw_ref[p] += dwt

    @pl.when(p == n_pair - 1)
    def _():
        for blk in range(NBLK):
            rows = slice(blk * HB, (blk + 1) * HB)
            dev, part = owner(blk)
            dkv_ref[dev, 0, part, :] = dckv[rows, :].astype(BF)
            for i in range(n_batch):
                @pl.when(b == i)
                def _():
                    dkpe_ref[dev, part, i * RD:(i + 1) * RD] = dkpe[rows, :].astype(BF)


def attention(rank, q, do, wk, wv, cos_t, sin_t, kv, kpe, prev, b0, nb):
    pair_blk = lambda w: pl.BlockSpec((1, QB, w), lambda b, p, *_: (b0 + b, 0, p))
    out_blk = lambda w: pl.BlockSpec((1, QB, w), lambda b, p, *_: (b, 0, p))
    w_blk = pl.BlockSpec((HB, QB), lambda b, p, *_: (p, 0))
    full = pl.BlockSpec((16, QB), lambda b, p, *_: (0, 0))
    kv_blk = pl.BlockSpec((NCP, 1, QB, QB), lambda b, p, *_: (0, b0 + b, 0, 0))
    dkv_blk = kv_blk
    anyspec = [pl.BlockSpec(memory_space=pl.ANY)] * len(prev)
    grid_spec = pltpu.PrefetchScalarGridSpec(
        num_scalar_prefetch=1,
        grid=(nb, NPAIR),
        in_specs=[pair_blk(QB), pair_blk(HB), w_blk, w_blk, full, full, kv_blk, pl.BlockSpec((NCP, QB, HB), lambda b, p, *_: (0, 0, 0))] + anyspec,
        out_specs=[out_blk(HB), pair_blk(QB), pl.BlockSpec((NPAIR, QB, QB), lambda b, p, *_: (0, 0, 0)), dkv_blk,
                   pl.BlockSpec((NCP, QB, nb * RD), lambda b, p, *_: (0, 0, 0))],
        scratch_shapes=[
            pltpu.VMEM((SEQ, QB), BF), pltpu.VMEM((QB, SEQ), BF), pltpu.VMEM((SEQ, KD), BF), pltpu.VMEM((SEQ, HB), BF),
            pltpu.VMEM((5, CH, QB), F32), pltpu.VMEM((5, CH, QB), F32),
            pltpu.VMEM((SEQ, KD), F32), pltpu.VMEM((SEQ, HB), F32),
            pltpu.VMEM((SEQ, QB), F32), pltpu.VMEM((SEQ, RD), F32),
            pltpu.VMEM((2, QB, KD), BF), pltpu.VMEM((2, QB, HB), BF),
        ])
    return pl.pallas_call(
        functools.partial(attn_kernel, b0, nb),
        grid_spec=grid_spec,
        out_shape=[jax.ShapeDtypeStruct((nb, QB, HV), BF), jax.ShapeDtypeStruct((4, QB, QW), BF), jax.ShapeDtypeStruct((NPAIR, QB, QB), F32),
                   jax.ShapeDtypeStruct((NCP, 4, QB, QB), BF),
                   jax.ShapeDtypeStruct((NCP, QB, nb * RD), BF)],
        compiler_params=pltpu.CompilerParams(vmem_limit_bytes=50 * 1024 * 1024),
        cost_estimate=pl.CostEstimate(flops=nb * 20_000_000_000, bytes_accessed=nb * 8_000_000, transcendentals=0),
        input_output_aliases={9: 1, 10: 3} if prev else {},
        name="attn",
    )(rank, q, do, wk, wv, cos_t, sin_t, kv, kpe, *prev)


def norm_pull(grad, vals, gain):
    rr = lax.rsqrt(jnp.mean(vals * vals, axis=-1, keepdims=True) + EPS)
    h = grad * gain
    mix = jnp.mean(h * vals, axis=-1, keepdims=True) * (rr * rr * rr)
    return rr * h - vals * mix, jnp.sum(grad * (vals * rr), axis=0, keepdims=True)


def plane_kernel(n_arr, reduce, gather, n_z, with_lat, *refs):
    ins, refs = refs[:n_arr], refs[n_arr:]
    if with_lat:
        lat, cq_ref, ckv_ref, gq_ref, gkv_ref, cos_ref, sin_ref, raw, gg = refs[:9]
        refs = refs[9:]
    outs, refs = refs[:n_arr], refs[n_arr:]
    r = lax.axis_index('cp')
    z = lax.axis_index('tp')
    send, recv, scratch = refs[0], refs[1], refs[2:]
    peers = {1: {'cp': r ^ 1}, 2: {'cp': r ^ 2}, 4: {'cp': r ^ 4}}
    barrier = pltpu.get_barrier_semaphore()
    targets = list(peers.values()) + [{'tp': lax.rem(z + d, NTP)} for d in range(1, NTP if with_lat else n_z)]
    for t in targets:
        pl.semaphore_signal(barrier, inc=1, device_id=t, device_id_type=pl.DeviceIdType.MESH)
    pl.semaphore_wait(barrier, len(targets))
    count = [0]
    started = []

    def copy(src, dst, target):
        k = count[0]
        count[0] += 1
        c = pltpu.make_async_remote_copy(src_ref=src, dst_ref=dst, send_sem=send.at[k], recv_sem=recv.at[k],
                                         device_id=target, device_id_type=pl.DeviceIdType.MESH)
        c.start()
        started.append(c)
        return c

    work = []
    for i in range(n_arr):
        w = {'in': ins[i], 'out': outs[i]}
        if reduce:
            w['rc'], w['sb'], w['rd'], w['rx'], w['ry'] = scratch[:5]
            scratch = scratch[5:]
            rows = w['rd'].shape[0]
        else:
            rows = ins[i].shape[0]
        w['g'] = outs[i]
        w['a'] = slice(0, (rows // 2 + RH - 1) // RH * RH)
        w['b'] = slice(w['a'].stop, rows)
        work.append(w)
    if with_lat:
        zr = scratch[0]
        z_in = [copy(lat.at[lax.rem(z + d, NTP)], zr.at[d - 1], {'tp': lax.rem(z + d, NTP)}) for d in range(1, NTP)]
    if reduce:
        for w in work:
            w['c'] = [None] * 4
        for k in (3, 1, 2, 0):
            for w in work:
                w['c'][k] = copy(w['in'].at[r ^ (2 * k + 1)], w['rc'].at[k], peers[1])

        def local(w, k):
            w['c'][k].wait_recv()
            return w['in'][r ^ (2 * k)].astype(F32) + w['rc'][k].astype(F32)

        for w in work:
            w['sb'][3] = local(w, 3).astype(BF)
            w['da'] = copy(w['sb'].at[3, w['a']], w['rd'].at[w['a']], peers[2])
            w['db'] = copy(w['sb'].at[3, w['b']], w['rd'].at[w['b']], peers[4])
        for w in work:
            w['sb'][1] = local(w, 1).astype(BF)
            w['xa'] = copy(w['sb'].at[1, w['a']], w['rx'].at[w['a']], peers[2])
            w['sb'][2] = local(w, 2).astype(BF)
            w['yb'] = copy(w['sb'].at[2, w['b']], w['ry'].at[w['b']], peers[4])
        for w in work:
            w['da'].wait_recv()
            w['sb'][2, w['a']] = (w['sb'][2, w['a']].astype(F32) + w['rd'][w['a']].astype(F32)).astype(BF)
            w['ya'] = copy(w['sb'].at[2, w['a']], w['ry'].at[w['a']], peers[4])
            w['db'].wait_recv()
            w['sb'][1, w['b']] = (w['sb'][1, w['b']].astype(F32) + w['rd'][w['b']].astype(F32)).astype(BF)
            w['xb'] = copy(w['sb'].at[1, w['b']], w['rx'].at[w['b']], peers[2])
        for w in work:
            base = local(w, 0)
            for name in ('xa', 'yb', 'ya', 'xb'):
                w[name].wait_recv()
            total = base + w['rx'][...].astype(F32) + w['ry'][...].astype(F32)
            if gather:
                w['g'][z * NCP * (n_z > 1) + r] = total.astype(BF)
            else:
                w['out'][...] = total
    elif gather:
        for w in work:
            w['g'][r] = w['in'][...]
    if gather:
        def fan(w, zz):
            own = w['g'].at[zz + r]
            return {'zz': zz, 2: copy(own, own, peers[2]), 4: copy(own, own, peers[4]), 1: copy(own, own, peers[1])}

        flows = []
        z_copies = []
        for w in work:
            if n_z > 1:
                own = w['g'].at[z * NCP + r]
                z_copies.append([copy(own, own, {'tp': lax.rem(z + d, NTP)}) for d in range(1, n_z)])
            flows.append([fan(w, z * NCP if n_z > 1 else 0)])
        if with_lat:
            for c in z_in:
                c.wait_recv()
            for i in range(4):
                rows = slice(i * HD, (i + 1) * HD)
                own = lat[z, rows, :].astype(F32)
                for d in range(NTP - 1):
                    own = own + zr[d, rows, :].astype(F32)
                g_cq, part_q = norm_pull(own[:, :QL], cq_ref[rows, :].astype(F32), gq_ref[...])
                g_ckv, part_kv = norm_pull(own[:, QL:TOK], ckv_ref[rows, :].astype(F32), gkv_ref[...])
                p1, p2 = own[:, TOK:TOK + RH], own[:, TOK + RH:ALL]
                cc, ss = cos_ref[rows, :], sin_ref[rows, :]
                raw[z, rows, :] = jnp.concatenate([g_cq, g_ckv, p1 * cc + p2 * ss, p2 * cc - p1 * ss, jnp.zeros((HD, DWW - ALL), F32)], axis=1).astype(BF)
                part = jnp.concatenate([part_q, part_kv], axis=1)
                gg[...] = part if i == 0 else gg[...] + part
            z_in = [copy(raw.at[z], raw.at[z], {'tp': lax.rem(z + d, NTP)}) for d in range(1, NTP)]
        for d in range(n_z):
            for i, w in enumerate(work):
                f = flows[i][d]
                gx, gy = w['g'].at[f['zz'] + (r ^ 2)], w['g'].at[f['zz'] + (r ^ 4)]
                f[2].wait_recv()
                f['dy'] = copy(gx.at[w['b']], gx.at[w['b']], peers[4])
                f['cx'] = copy(gx, gx, peers[1])
                f[4].wait_recv()
                f['dx'] = copy(gy.at[w['a']], gy.at[w['a']], peers[2])
                f['cy'] = copy(gy, gy, peers[1])
                if d + 1 < n_z:
                    z_copies[i][d].wait_recv()
                    flows[i].append(fan(w, lax.rem(z + NTP - (d + 1), NTP) * NCP))
        for d in range(n_z):
            for i, w in enumerate(work):
                f = flows[i][d]
                f['dy'].wait_recv()
                f['dx'].wait_recv()
                gd = w['g'].at[f['zz'] + (r ^ 6)]
                f['cd'] = copy(gd, gd, peers[1])
        for d in range(n_z):
            for i, w in enumerate(work):
                f = flows[i][d]
                for name in (1, 'cx', 'cy', 'cd'):
                    f[name].wait_recv()
        if with_lat:
            for c in z_in:
                c.wait_recv()
    for c in started:
        c.wait_send()


def plane(arrs, cid, reduce, gather, n_z=1, extra=()):
    scratch, shapes = [], []
    n_copy = 0
    for v in arrs:
        n, m = v.shape[-2:]
        if reduce:
            scratch += [pltpu.VMEM((4, n, m), BF), pltpu.VMEM((4, n, m), BF)] + [pltpu.VMEM((n, m), BF)] * 3
            n_copy += 10
        if gather:
            shapes.append(jax.ShapeDtypeStruct((NCP * n_z, n, m), BF))
            n_copy += 8 * n_z + n_z - 1
        else:
            shapes.append(jax.ShapeDtypeStruct((n, m), F32))
    vmem = pl.BlockSpec(memory_space=pltpu.VMEM)
    if extra:
        shapes = [jax.ShapeDtypeStruct((4, QB, DWW), BF), jax.ShapeDtypeStruct((1, TOK), F32)] + shapes
        scratch.append(pltpu.VMEM((3, QB, DWW), BF))
        n_copy += 6
    return pl.pallas_call(
        functools.partial(plane_kernel, len(arrs), reduce, gather, n_z, bool(extra)),
        out_shape=shapes,
        in_specs=[vmem] * (len(arrs) + len(extra)),
        out_specs=[vmem] * len(shapes),
        scratch_shapes=[pltpu.SemaphoreType.DMA((n_copy,)), pltpu.SemaphoreType.DMA((n_copy,))] + scratch,
        compiler_params=pltpu.CompilerParams(collective_id=cid, has_side_effects=True, vmem_limit_bytes=60 * TOK * TOK),
        cost_estimate=pl.CostEstimate(flops=30_000_000_000, bytes_accessed=10_000_000, transcendentals=0),
        name="plane",
    )(*arrs, *extra)


def zshift(v, d):
    return lax.ppermute(v, 'tp', [(i, (i + d) % NTP) for i in range(NTP)])


def zrel(v):
    return [v] + [zshift(v, d) for d in range(1, NTP)]


def norm_f32(raw_vals, gain_vec):
    inv_rms = lax.rsqrt(jnp.mean(raw_vals * raw_vals, axis=-1, keepdims=True) + EPS)
    return raw_vals * inv_rms * gain_vec


def solution(mesh):
    def per_device(hidden, grad_out, w_dq, g_q, w_dkv, g_kv, w_uq, w_uk, w_uv, w_o):
        rank = lax.axis_index('cp')
        z = lax.axis_index('tp')
        x2 = hidden.reshape(TOK, DM)
        dy2 = grad_out.reshape(TOK, DM)
        half = 16
        inv_freq = 1.0 / (THETA ** (jnp.arange(half, dtype=F32) * 2.0 / 32))
        idx = jnp.arange(QB, dtype=jnp.int32)
        positions = jnp.where(idx < HB, rank, NBLK - 1 - rank) * HB + idx % HB
        angles = positions.astype(F32)[:, None] * inv_freq[None, :]
        cos_tab, sin_tab = jnp.cos(angles), jnp.sin(angles)
        cos_t, sin_t = cos_tab.T, sin_tab.T
        gq = g_q.astype(F32)
        gkv = g_kv.astype(F32)

        kv_raw = dot(x2, w_dkv, NN).astype(BF)
        ckv_f32 = kv_raw[:, :QB].astype(F32)
        c_kv = norm_f32(ckv_f32, gkv).astype(BF)
        pe = kv_raw[:, QB:].astype(F32).reshape(4, QB, 32)
        pe1, pe2 = pe[..., :half], pe[..., half:]
        k_pe = jnp.concatenate([pe1 * cos_tab - pe2 * sin_tab, pe2 * cos_tab + pe1 * sin_tab], axis=-1).astype(BF)
        kv, kpe = plane([c_kv, k_pe.transpose(1, 0, 2).reshape(QB, HB)], 0, False, True)
        kv = kv.reshape(NCP, 4, QB, QB)

        wo2 = w_o.reshape(HV, DM)
        wo_rel = jnp.stack(zrel(lax.dynamic_slice_in_dim(wo2, rank * 80, 80, 0)))
        wo_rel, kv = lax.optimization_barrier((wo_rel, kv))
        wo_rel = lax.all_gather(wo_rel, 'cp', axis=1, tiled=True).reshape(DM, DM)

        cq_raw = dot(x2, w_dq, NN).astype(BF)
        cq_f32 = cq_raw.astype(F32)
        c_q = norm_f32(cq_f32, gq).astype(BF)
        w_qt = w_uq.transpose(1, 2, 0)
        w_q = jnp.concatenate([w_qt[:, :HD].reshape(NPAIR, HB, QL), w_qt[:, HD:].reshape(NPAIR, HD, QL), jnp.zeros((NPAIR, HD, QL), BF)], axis=1).reshape(QW, QL)
        q = dot(c_q, w_q, NT).astype(BF).reshape(4, QB, QW)
        do = dot(dy2, wo2, NT).astype(BF).reshape(4, QB, HV)
        wk = w_uk.transpose(1, 2, 0).reshape(HV, QB)
        wv = w_uv.transpose(1, 2, 0).reshape(HV, QB)

        n_split = 4
        nb = 4 // n_split
        runs = []
        for i in range(n_split):
            prev = [runs[-1][1], runs[-1][3]] if runs else []
            runs.append(attention(rank.reshape(1), q, do, wk, wv, cos_t, sin_t, kv, kpe, prev, i * nb, nb))
        o_rel = []
        for run in runs:
            parts = [run[0]]
            for d in range(1, NTP):
                parts.append(zshift(run[0], d))
            o_rel.append(jnp.concatenate(parts, axis=2))
        o_rel = jnp.concatenate(o_rel, axis=0).reshape(TOK, DM)
        o = jnp.concatenate([run[0] for run in runs], axis=0).reshape(TOK, HV)
        dq = runs[-1][1].reshape(TOK, QW)
        dwkv = sum(run[2] for run in runs)

        dckv, *dkpe = plane([runs[-1][3].reshape(NCP, TOK, QB)] + [run[4] for run in runs], 1, True, False)
        dkpe = jnp.concatenate(dkpe, axis=1).reshape(QB, 4, RD).transpose(1, 0, 2)
        lat_q = dot(dq, w_q, NN).reshape(4, QB, QL)
        lat = jnp.concatenate([lat_q.astype(BF), dckv.reshape(4, QB, QB).astype(BF), dkpe.astype(BF), jnp.zeros((4, QB, DWW - ALL), BF)], axis=-1)
        cq_own = lax.dynamic_slice_in_dim(cq_raw, z * QB, QB, 0)
        ckv_own = lax.dynamic_slice_in_dim(kv_raw, z * QB, QB, 0)[:, :QB]
        dwq = dot(dq, c_q, TN).astype(BF).reshape(NCP, KD, QL)
        dwkv = dwkv.reshape(NCP, KD, QB).astype(BF)
        dwo = dot(o, dy2, TN).astype(BF).reshape(NCP, 80, DM)
        raw, grad_g, dwq, dwkv, dwo = plane([dwq, dwkv, dwo], 3, True, True, 1, [lat, cq_own, ckv_own, gq[None], gkv[None], cos_tab, sin_tab])
        raw_all = raw.reshape(TOK, DWW)[:, :ALL]

        grad_g = jnp.pad(grad_g.reshape(HB, NCP).astype(BF), ((0, HV - HB), (0, DWW - ALL - NCP)))
        x_slice = lax.dynamic_slice_in_dim(x2, z * HV, HV, 1)
        dwd = jnp.concatenate([dot(x_slice, raw_all, TN).astype(BF), grad_g], axis=1).reshape(NCP, 80, DWW)
        dwd, = plane([dwd], 2, True, True, NTP)
        dwd = dwd.reshape(DM, DWW)
        grad_g = jnp.sum(dwd.reshape(NTP, HV, DWW)[:, :HB, ALL:ALL + NCP].astype(F32), axis=0).reshape(TOK)
        grad_hidden = (dot(raw_all[:, :QL], w_dq, NT) + dot(raw_all[:, QL:], w_dkv, NT)).astype(BF).reshape(4, QB, DM)
        attn_out = dot(o_rel, wo_rel, NN).astype(BF).reshape(4, QB, DM)

        dwq = dwq.reshape(NPAIR, QB, QL).astype(F32)
        grad_uq = jnp.concatenate([dwq[:, :HB].reshape(10, HD, QL), dwq[:, HB:HB + HD].reshape(10, RD, QL)], axis=1).transpose(2, 0, 1)
        dwkv = dwkv.reshape(NPAIR, QB, QB).astype(F32)
        grad_uk = dwkv[:, :HB].reshape(10, HD, QB).transpose(2, 0, 1)
        grad_uv = dwkv[:, HB:].reshape(10, HD, QB).transpose(2, 0, 1)
        return (attn_out, grad_hidden, dwd[:, :QL].astype(F32), grad_g[:QL], dwd[:, QL:ALL].astype(F32), grad_g[QL:], grad_uq, grad_uk, grad_uv, dwo.reshape(HV, DM).astype(F32).reshape(10, HD, DM))

    seq_spec = P(None, 'cp', None)
    full_spec = P()
    head_spec = P(None, 'tp', None)
    out_head_spec = P('tp', None, None)
    all_specs = (seq_spec, seq_spec, full_spec, full_spec, full_spec, full_spec, head_spec, head_spec, head_spec, out_head_spec)
    return jax.shard_map(per_device, mesh=mesh, in_specs=all_specs, out_specs=all_specs, check_vma=False)
```

```python
import functools
import math

import jax
import jax.numpy as jnp
from jax import lax
from jax.experimental import pallas as pl
from jax.experimental.pallas import tpu as pltpu
from jax.sharding import PartitionSpec as P


EPS = 1e-6
THETA = 10000.0
NEG_BIG = -1e30
BF = jnp.bfloat16
F32 = jnp.float32
NT = (((1,), (1,)), ((), ()))
TN = (((0,), (0,)), ((), ()))
NN = (((1,), (0,)), ((), ()))
HB, QB, CH, SEQ = 128, 256, 512, 2048
HD, KD, RD, QL = 64, 160, 32, 768
NBLK, NCP, NTP, NPAIR = 16, 8, 4, 5
TOK, DM, HV, QW, ALL, DWW = 1024, 2560, 640, 1280, 1056, 1152
RH = 16
HOPS = range(1, NTP)


def dot(a, b, dims):
    return lax.dot_general(a, b, dims, preferred_element_type=F32)


def owner(blk):
    if blk < NCP:
        return blk, slice(0, HB)
    return NBLK - 1 - blk, slice(HB, QB)


def attn_kernel(b0, r_ref, q_ref, do_ref, wk_ref, wv_ref, cos_ref, sin_ref, *rest):
    kv_ref, kpe_ref = rest[:2]
    if b0 > 0:
        old_ref = rest[2]
    rest = rest[2 if b0 == 0 else 5:]
    o_ref, dq_ref, dw_ref, dkv_ref, dkpe_ref, ckv, ckvt, kcat, vv, s_scr, dp_scr, dk_acc, dv_acc, dckv, dkpe, qbd, dobd = rest
    b = pl.program_id(0)
    p = pl.program_id(1)
    n_pair = pl.num_programs(1)
    r = r_ref[0]
    scale = 96.0 ** -0.5
    c2 = scale * math.log2(math.e)

    @pl.when(p == 0)
    def _():
        for blk in range(NBLK):
            rows = slice(blk * HB, (blk + 1) * HB)
            dev, part = owner(blk)
            ckv[rows, :] = kv_ref[dev, 0, part, :]
            kcat[rows, HB:KD] = kpe_ref[dev, part, b0 * RD:(b0 + 1) * RD]
        for i in range(4):
            ckvt[:, i * CH:(i + 1) * CH] = ckv[i * CH:(i + 1) * CH, :].T
        dckv[...] = jnp.zeros_like(dckv)
        dkpe[...] = jnp.zeros_like(dkpe)

    wkv = jnp.concatenate([wk_ref[...], wv_ref[...]], axis=0)
    for i in range(4):
        rows = slice(i * CH, (i + 1) * CH)
        kv = dot(ckv[rows, :], wkv, NT).astype(BF)
        kcat[rows, 0:HB] = kv[:, 0:HB]
        vv[rows, :] = kv[:, HB:QB]

    cos_t = cos_ref[...]
    sin_t = sin_ref[...]
    lane = lax.broadcasted_iota(jnp.int32, (HB, HB), 1)
    zero = jnp.zeros((HB, HB), BF)
    qpt = q_ref[0, :, HB:QB].astype(F32).T
    roped = []
    for h in range(2):
        u1 = qpt[h * 32:h * 32 + 16, :]
        u2 = qpt[h * 32 + 16:h * 32 + 32, :]
        roped.append(u1 * cos_t - u2 * sin_t)
        roped.append(u2 * cos_t + u1 * sin_t)
    qpe = jnp.concatenate(roped + [jnp.zeros((HD, QB), F32)], axis=0).T.astype(BF)
    for s in range(2):
        rows = slice(s * HB, (s + 1) * HB)
        qn = q_ref[0, rows, 0:HB]
        gg = do_ref[0, rows, :]
        qbd[s, 0:HB, 0:HB] = jnp.where(lane < HD, qn, zero)
        qbd[s, HB:QB, 0:HB] = jnp.where(lane < HD, zero, qn)
        qbd[s, 0:HB, HB:KD] = qpe[rows, 0:32]
        qbd[s, HB:QB, HB:KD] = qpe[rows, 32:64]
        dobd[s, 0:HB, :] = jnp.where(lane < HD, gg, zero)
        dobd[s, HB:QB, :] = jnp.where(lane < HD, zero, gg)

    low = r < 4
    sel3 = jnp.where(low, 1, 0)
    chunks = [(1, 0), (1, 1), (1, 2), (sel3, jnp.where(low, 3, 0)), (0, jnp.where(low, 0, 1))]

    def keys(c):
        kc = chunks[c][1]
        if isinstance(kc, int):
            return slice(kc * CH, (kc + 1) * CH)
        return pl.ds(pl.multiple_of(kc * CH, CH), CH)

    diff = (lax.broadcasted_iota(jnp.int32, (CH, QB), 0)
            - lax.rem(lax.broadcasted_iota(jnp.int32, (CH, QB), 1), HB))
    maxes = []
    for c in range(5):
        sel, kc = chunks[c]
        s = dot(kcat[keys(c), :], qbd[sel], NT)
        if c >= 2:
            blk = jnp.where(sel == 1, 15 - r, r)
            s = jnp.where(diff <= blk * HB - kc * CH, s, NEG_BIG)
        s_scr[c] = s
        maxes.append(jnp.max(s, axis=0, keepdims=True))

    def join(vals, op, ident):
        ident = jnp.full_like(vals[3], ident)
        top = op(op(op(vals[0], vals[1]), vals[2]), jnp.where(low, vals[3], ident))
        bot = op(vals[4], jnp.where(low, ident, vals[3]))
        return [top, top, top, jnp.where(low, top, bot), bot]

    m = join(maxes, jnp.maximum, NEG_BIG)
    sums, dots = [], []
    for c in range(5):
        sel, kc = chunks[c]
        e = jnp.exp2((s_scr[c] - m[c]) * c2)
        s_scr[c] = e
        sums.append(jnp.sum(e, axis=0, keepdims=True))
        dp = dot(vv[keys(c), :], dobd[sel], NT)
        dp_scr[c] = dp
        dots.append(jnp.sum(e * dp, axis=0, keepdims=True))
    total = join(sums, jnp.add, 0.0)
    inv = [1.0 / t for t in total]
    dsum = join(dots, jnp.add, 0.0)
    delta = [d * i for d, i in zip(dsum, inv)]
    ots, dqts = [], []
    dk_acc[3 * CH:SEQ, :] = jnp.zeros((CH, KD), F32)
    dv_acc[3 * CH:SEQ, :] = jnp.zeros((CH, HB), F32)
    for c in range(5):
        sel, kc = chunks[c]
        pr = s_scr[c] * inv[c]
        pb = pr.astype(BF)
        ds = (pr * (dp_scr[c] - delta[c])).astype(BF)
        ots.append(dot(vv[keys(c), :], pb, TN))
        dqts.append(dot(kcat[keys(c), :], ds, TN))
        dv = dot(pb, dobd[sel], NN)
        dk = dot(ds, qbd[sel], NN)
        if c < 3:
            dk_acc[keys(c), :] = dk
            dv_acc[keys(c), :] = dv
        else:
            dk_acc[keys(c), :] += dk
            dv_acc[keys(c), :] += dv
    ot = join(ots, jnp.add, 0.0)
    dqt = join(dqts, jnp.add, 0.0)
    for s in range(2):
        rows = slice(s * HB, (s + 1) * HB)
        a = ot[0 if s == 1 else 4]
        o_ref[0, rows, :] = jnp.concatenate([a[0:HD, 0:HB], a[HD:HB, HB:QB]], axis=0).T.astype(BF)
        g = dqt[0 if s == 1 else 4] * scale
        dq_ref[0, rows, 0:HB] = jnp.concatenate([g[0:HD, 0:HB], g[HD:HB, HB:QB]], axis=0).T.astype(BF)
        pe = []
        for h in range(2):
            g1 = g[128:144, h * HB:(h + 1) * HB]
            g2 = g[144:160, h * HB:(h + 1) * HB]
            ct = cos_t[:, rows]
            st = sin_t[:, rows]
            pe.append(g1 * ct + g2 * st)
            pe.append(g2 * ct - g1 * st)
        dq_ref[0, rows, HB:QB] = jnp.concatenate(pe + [jnp.zeros((HD, HB), F32)], axis=0).T.astype(BF)

    dwt = jnp.zeros((QB, QB), F32)
    for i in range(4):
        rows = slice(i * CH, (i + 1) * CH)
        dkv = jnp.concatenate([(dk_acc[rows, 0:HB] * scale).astype(BF), dv_acc[rows, :].astype(BF)], axis=1)
        dkpe[rows, :] += dk_acc[rows, HB:KD] * scale
        dckv[rows, :] += dot(dkv, wkv, NN)
        dwt = dwt + dot(ckvt[:, rows], dkv, NN)
    dwt = dwt.T

    @pl.when(b == 0)
    def _():
        dw_ref[p] = dwt

    @pl.when(b > 0)
    def _():
        dw_ref[p] += dwt

    @pl.when(p == n_pair - 1)
    def _():
        for blk in range(NBLK):
            rows = slice(blk * HB, (blk + 1) * HB)
            dev, part = owner(blk)
            dkv_ref[dev, 0, part, :] = dckv[rows, :].astype(BF)
            piece = dkpe[rows, :].astype(BF)
            if b0 > 0:
                dkpe_ref[dev, part, :] = old_ref[dev, part, :]
            dkpe_ref[dev, part, b0 * RD:(b0 + 1) * RD] = piece


def attention(rank, q, do, wk, wv, cos_t, sin_t, kv, kpe, prev, b0, nb):
    pair_blk = lambda w: pl.BlockSpec((1, QB, w), lambda b, p, *_: (b0 + b, 0, p))
    out_blk = lambda w: pl.BlockSpec((1, QB, w), lambda b, p, *_: (b, 0, p))
    w_blk = pl.BlockSpec((HB, QB), lambda b, p, *_: (p, 0))
    full = pl.BlockSpec((16, QB), lambda b, p, *_: (0, 0))
    kv_blk = pl.BlockSpec((NCP, 1, QB, QB), lambda b, p, *_: (0, b0 + b, 0, 0))
    dkv_blk = kv_blk
    pe_blk = pl.BlockSpec((NCP, QB, HB), lambda b, p, *_: (0, 0, 0))
    anyspec = [pe_blk] + [pl.BlockSpec(memory_space=pl.ANY)] * 2 if prev else []
    grid_spec = pltpu.PrefetchScalarGridSpec(
        num_scalar_prefetch=1,
        grid=(nb, NPAIR),
        in_specs=[pair_blk(QB), pair_blk(HB), w_blk, w_blk, full, full, kv_blk, pe_blk] + anyspec,
        out_specs=[out_blk(HB), pair_blk(QB), pl.BlockSpec((NPAIR, QB, QB), lambda b, p, *_: (0, 0, 0)), dkv_blk,
                   pe_blk],
        scratch_shapes=[
            pltpu.VMEM((SEQ, QB), BF), pltpu.VMEM((QB, SEQ), BF), pltpu.VMEM((SEQ, KD), BF), pltpu.VMEM((SEQ, HB), BF),
            pltpu.VMEM((5, CH, QB), F32), pltpu.VMEM((5, CH, QB), F32),
            pltpu.VMEM((SEQ, KD), F32), pltpu.VMEM((SEQ, HB), F32),
            pltpu.VMEM((SEQ, QB), F32), pltpu.VMEM((SEQ, RD), F32),
            pltpu.VMEM((2, QB, KD), BF), pltpu.VMEM((2, QB, HB), BF),
        ])
    return pl.pallas_call(
        functools.partial(attn_kernel, b0),
        grid_spec=grid_spec,
        out_shape=[jax.ShapeDtypeStruct((nb, QB, HV), BF), jax.ShapeDtypeStruct((4, QB, QW), BF), jax.ShapeDtypeStruct((NPAIR, QB, QB), F32),
                   jax.ShapeDtypeStruct((NCP, 4, QB, QB), BF),
                   jax.ShapeDtypeStruct((NCP, QB, HB), BF)],
        compiler_params=pltpu.CompilerParams(vmem_limit_bytes=50 * TOK * TOK),
        cost_estimate=pl.CostEstimate(flops=nb * 20_000_000_000, bytes_accessed=nb * 8_000_000, transcendentals=0),
        input_output_aliases={10: 1, 11: 3} if prev else {},
        name="attn",
    )(rank, q, do, wk, wv, cos_t, sin_t, kv, kpe, *prev)


def norm_pull(grad, vals, gain):
    rr = lax.rsqrt(jnp.mean(vals * vals, axis=-1, keepdims=True) + EPS)
    h = grad * gain
    mix = jnp.mean(h * vals, axis=-1, keepdims=True) * (rr * rr * rr)
    return rr * h - vals * mix, jnp.sum(grad * (vals * rr), axis=0, keepdims=True)


class Filler:
    def __init__(self, filler, refs):
        n_in, n_out, n_extra = len(filler.args), len(filler.outs), len(filler.extra)
        src, self.outs, refs = refs[:n_in], refs[n_in:n_in + n_out], refs[n_in + n_out:]
        self.bufs, sems, extra = refs[:n_in], refs[n_in], refs[n_in + 1:n_in + 1 + n_extra]
        self.loads = [pltpu.make_async_copy(a, b, sems.at[i]) for i, (a, b) in enumerate(zip(src, self.bufs))]
        for c in self.loads:
            c.start()
        self.ready = [False] * n_in
        self.groups = [list(g) for g in filler.groups(self, self.bufs, self.outs, extra)]

    def need(self, which):
        for i in which:
            if not self.ready[i]:
                self.ready[i] = True
                self.loads[i].wait()

    def run(self, k):
        while k > 0 and self.groups:
            which, prep, body, lo, hi = self.groups[0]
            self.need(which)
            if prep is not None:
                prep()
            n = min(k, hi - lo)

            def step(t, carry):
                body(t)
                return carry

            lax.fori_loop(lo, lo + n, step, 0)
            k -= n
            if lo + n == hi:
                self.groups.pop(0)
            else:
                self.groups[0] = [which, None, body, lo + n, hi]


class NoFill:
    def run(self, k):
        return None


class Spec:
    def __init__(self, args, outs, extra, groups):
        self.args, self.outs, self.extra, self.groups = args, outs, extra, groups


def tile(t, n):
    return pl.ds(pl.multiple_of(t * n, n), n)


def plane_kernel(n_arr, reduce, gather, n_z, with_lat, filler, *refs):
    ins, refs = refs[:n_arr], refs[n_arr:]
    n_fill = len(filler.args) if filler else 0
    if with_lat:
        lat, cq_ref, ckv_ref, gq_ref, gkv_ref, cos_ref, sin_ref = refs[:7]
        refs = refs[7:]
    fill_src, refs = refs[:n_fill], refs[n_fill:]
    if with_lat:
        (raw, gg), refs = refs[:2], refs[2:]
    outs, refs = refs[:n_arr], refs[n_arr:]
    fill_out, refs = (refs[:len(filler.outs)], refs[len(filler.outs):]) if filler else ((), refs)
    r = lax.axis_index('cp')
    z = lax.axis_index('tp')
    send, recv, scratch = refs[0], refs[1], refs[2:]
    peers = {m: {'cp': r ^ m} for m in (1, 2, 4)}
    barrier = pltpu.get_barrier_semaphore()
    targets = list(peers.values()) + [{'tp': lax.rem(z + d, NTP)} for d in range(1, NTP if with_lat else n_z)]
    for t in targets:
        pl.semaphore_signal(barrier, inc=1, device_id=t, device_id_type=pl.DeviceIdType.MESH)
    pl.semaphore_wait(barrier, len(targets))
    count = [0]
    started = []
    n_tail = (len(filler.args) + 1 + len(filler.extra)) if filler else 0
    fill = Filler(filler, list(fill_src) + list(fill_out) + list(scratch[len(scratch) - n_tail:])) if filler else NoFill()

    def copy(src, dst, target):
        k = count[0]
        count[0] += 1
        c = pltpu.make_async_remote_copy(src_ref=src, dst_ref=dst, send_sem=send.at[k], recv_sem=recv.at[k],
                                         device_id=target, device_id_type=pl.DeviceIdType.MESH)
        c.start()
        started.append(c)
        return c

    work = []
    for i in range(n_arr):
        w = {'in': ins[i], 'out': outs[i]}
        if reduce:
            w['rc'], w['sb'], w['rd'], w['rx'], w['ry'] = scratch[:5]
            scratch = scratch[5:]
            rows = w['rd'].shape[0]
        else:
            rows = ins[i].shape[0]
        w['g'] = outs[i]
        w['a'] = slice(0, (rows // 2 + RH - 1) // RH * RH)
        w['b'] = slice(w['a'].stop, rows)
        work.append(w)
    if with_lat:
        zr = scratch[0]
        z_in = [copy(lat.at[lax.rem(z + d, NTP)], zr.at[d - 1], {'tp': lax.rem(z + d, NTP)}) for d in HOPS]
    if reduce:
        for w in work:
            w['c'] = [None] * 4
        for k in (3, 1, 2, 0):
            for w in work:
                w['c'][k] = copy(w['in'].at[r ^ (2 * k + 1)], w['rc'].at[k], peers[1])

        fill.run(8)

        def local(w, k):
            w['c'][k].wait_recv()
            return w['in'][r ^ (2 * k)].astype(F32) + w['rc'][k].astype(F32)

        for w in work:
            w['sb'][3] = local(w, 3).astype(BF)
            w['da'] = copy(w['sb'].at[3, w['a']], w['rd'].at[w['a']], peers[2])
            w['db'] = copy(w['sb'].at[3, w['b']], w['rd'].at[w['b']], peers[4])
        fill.run(4)
        for w in work:
            w['sb'][1] = local(w, 1).astype(BF)
            w['xa'] = copy(w['sb'].at[1, w['a']], w['rx'].at[w['a']], peers[2])
            w['sb'][2] = local(w, 2).astype(BF)
            w['yb'] = copy(w['sb'].at[2, w['b']], w['ry'].at[w['b']], peers[4])
        fill.run(4)
        for w in work:
            w['da'].wait_recv()
            w['sb'][2, w['a']] = (w['sb'][2, w['a']].astype(F32) + w['rd'][w['a']].astype(F32)).astype(BF)
            w['ya'] = copy(w['sb'].at[2, w['a']], w['ry'].at[w['a']], peers[4])
            w['db'].wait_recv()
            w['sb'][1, w['b']] = (w['sb'][1, w['b']].astype(F32) + w['rd'][w['b']].astype(F32)).astype(BF)
            w['xb'] = copy(w['sb'].at[1, w['b']], w['rx'].at[w['b']], peers[2])
        fill.run(6)
        for w in work:
            base = local(w, 0)
            for name in ('xa', 'yb', 'ya', 'xb'):
                w[name].wait_recv()
            total = base + w['rx'][...].astype(F32) + w['ry'][...].astype(F32)
            if gather:
                w['g'][z * NCP * (n_z > 1) + r] = total.astype(BF)
            else:
                w['out'][...] = total
    elif gather:
        for w in work:
            w['g'][r] = w['in'][...]
    if gather:
        def fan(w, zz):
            own = w['g'].at[zz + r]
            return {'zz': zz, 2: copy(own, own, peers[2]), 4: copy(own, own, peers[4]), 1: copy(own, own, peers[1])}

        flows = []
        z_copies = []
        for w in work:
            if n_z > 1:
                own = w['g'].at[z * NCP + r]
                z_copies.append([copy(own, own, {'tp': lax.rem(z + d, NTP)}) for d in range(1, n_z)])
            flows.append([fan(w, z * NCP if n_z > 1 else 0)])
        if with_lat:
            fill.run(10)
            for c in z_in:
                c.wait_recv()
            for i in range(4):
                rows = slice(i * HD, (i + 1) * HD)
                own = lat[z, rows, :].astype(F32)
                for d in range(NTP - 1):
                    own = own + zr[d, rows, :].astype(F32)
                g_cq, part_q = norm_pull(own[:, :QL], cq_ref[rows, :].astype(F32), gq_ref[...])
                g_ckv, part_kv = norm_pull(own[:, QL:TOK], ckv_ref[rows, :].astype(F32), gkv_ref[...])
                p1, p2 = own[:, TOK:TOK + RH], own[:, TOK + RH:ALL]
                cc, ss = cos_ref[rows, :], sin_ref[rows, :]
                raw[z, rows, :] = jnp.concatenate([g_cq, g_ckv, p1 * cc + p2 * ss, p2 * cc - p1 * ss, jnp.zeros((HD, DWW - ALL), F32)], axis=1).astype(BF)
                part = jnp.concatenate([part_q, part_kv], axis=1)
                gg[...] = part if i == 0 else gg[...] + part
            z_in = [copy(raw.at[z], raw.at[z], {'tp': lax.rem(z + d, NTP)}) for d in HOPS]
        for d in range(n_z):
            fill.run(4)
            for i, w in enumerate(work):
                f = flows[i][d]
                gx, gy = w['g'].at[f['zz'] + (r ^ 2)], w['g'].at[f['zz'] + (r ^ 4)]
                f[2].wait_recv()
                f['dy'] = copy(gx.at[w['b']], gx.at[w['b']], peers[4])
                f['cx'] = copy(gx, gx, peers[1])
                f[4].wait_recv()
                f['dx'] = copy(gy.at[w['a']], gy.at[w['a']], peers[2])
                f['cy'] = copy(gy, gy, peers[1])
                if d + 1 < n_z:
                    z_copies[i][d].wait_recv()
                    flows[i].append(fan(w, lax.rem(z + NTP - (d + 1), NTP) * NCP))
        fill.run(3)
        for d in range(n_z):
            for i, w in enumerate(work):
                f = flows[i][d]
                f['dy'].wait_recv()
                f['dx'].wait_recv()
                gd = w['g'].at[f['zz'] + (r ^ 6)]
                f['cd'] = copy(gd, gd, peers[1])
        fill.run(QB)
        for d in range(n_z):
            for i, w in enumerate(work):
                f = flows[i][d]
                for name in (1, 'cx', 'cy', 'cd'):
                    f[name].wait_recv()
        if with_lat:
            for c in z_in:
                c.wait_recv()
    fill.run(QB)
    for c in started:
        c.wait_send()


def plane(arrs, cid, reduce, gather, n_z=1, extra=(), filler=None):
    scratch, shapes = [], []
    n_copy = 0
    for v in arrs:
        n, m = v.shape[-2:]
        if reduce:
            scratch += [pltpu.VMEM((4, n, m), BF), pltpu.VMEM((4, n, m), BF)] + [pltpu.VMEM((n, m), BF)] * 3
            n_copy += 10
        if gather:
            shapes.append(jax.ShapeDtypeStruct((NCP * n_z, n, m), BF))
            n_copy += 8 * n_z + n_z - 1
        else:
            shapes.append(jax.ShapeDtypeStruct((n, m), F32))
    vmem = pl.BlockSpec(memory_space=pltpu.VMEM)
    if extra:
        shapes = [jax.ShapeDtypeStruct((4, QB, DWW), BF), jax.ShapeDtypeStruct((1, TOK), F32)] + shapes
        scratch.append(pltpu.VMEM((3, QB, DWW), BF))
        n_copy += 6
    anyspec = []
    fill_args = ()
    if filler:
        fill_args = filler.args
        shapes += filler.outs
        anyspec = [pl.BlockSpec(memory_space=pl.ANY)] * len(filler.args)
        scratch += [pltpu.VMEM(a.shape, BF) for a in filler.args] + [pltpu.SemaphoreType.DMA((len(filler.args),))] + filler.extra
    return pl.pallas_call(
        functools.partial(plane_kernel, len(arrs), reduce, gather, n_z, bool(extra), filler),
        out_shape=shapes,
        in_specs=[vmem] * (len(arrs) + len(extra)) + anyspec,
        out_specs=[vmem] * len(shapes),
        scratch_shapes=[pltpu.SemaphoreType.DMA((n_copy,)), pltpu.SemaphoreType.DMA((n_copy,))] + scratch,
        compiler_params=pltpu.CompilerParams(collective_id=cid, has_side_effects=True, vmem_limit_bytes=60 * TOK * TOK),
        cost_estimate=pl.CostEstimate(flops=30_000_000_000, bytes_accessed=TOK * TOK, transcendentals=0),
        name="plane",
    )(*arrs, *extra, *fill_args)


def sds(*shape):
    return jax.ShapeDtypeStruct(shape, BF)


def front_fill(x2, w_dq, gq, dy2, wo2, w_q):
    def groups(f, bufs, outs, extra):
        x, wd, dy, wo, wq, gain = bufs
        do, cq_raw, c_q, q = outs

        def do_body(t):
            do[tile(t, QB), :] = dot(dy[tile(t, QB), :], wo[...], NT).astype(BF)

        def q_body(t):
            u = dot(x[tile(t, QB), :], wd[...], NN).astype(BF)
            cq_raw[tile(t, QB), :] = u
            c = norm_f32(u.astype(F32), gain[...].astype(F32)).astype(BF)
            c_q[tile(t, QB), :] = c
            q[tile(t, QB), :] = dot(c, wq[...], NT).astype(BF)

        return [((2, 3), None, do_body, 0, 4), ((0, 1, 4, 5), None, q_body, 0, 4)]

    return Spec([x2, w_dq, dy2, wo2, w_q, gq[None]], [sds(TOK, HV), sds(TOK, QL), sds(TOK, QL), sds(TOK, QW)], [], groups)


def mid_fill(dq, w_q, o, dy2, c_q):
    def groups(f, bufs, outs, extra):
        dqv, wq, ov, dy, cq = bufs
        lat_q, dwo, dwq = outs
        ot, dqt = extra

        def lat_body(t):
            lat_q[tile(t, QB), :] = dot(dqv[tile(t, QB), :], wq[...], NN).astype(BF)

        def turn_o(t):
            ot[:, tile(t, QB)] = ov[tile(t, QB), :].T

        def dwo_body(t):
            dwo[:, tile(t, QB)] = dot(ot[...], dy[:, tile(t, QB)], NN).astype(BF)

        def turn_dq(t):
            dqt[:, tile(t, QB)] = dqv[tile(t, QB), :].T

        def dwq_body(t):
            dwq[:, tile(t, QB)] = dot(dqt[...], cq[:, tile(t, QB)], NN).astype(BF)

        return [((0, 1), None, lat_body, 0, 4), ((2,), None, turn_o, 0, 4), ((3,), None, dwo_body, 0, 10),
                ((), None, turn_dq, 0, 4), ((4,), None, dwq_body, 0, 3)]

    return Spec([dq, w_q, o, dy2, c_q], [sds(TOK, QL), sds(HV, DM), sds(QW, QL)], [pltpu.VMEM((HV, TOK), BF), pltpu.VMEM((QW, TOK), BF)], groups)


def y_fill(o_rel, wo_rel):
    def groups(f, bufs, outs, extra):
        ov, wo = bufs
        y, = outs

        def y_body(t):
            rows, cols = tile(lax.rem(t, 2), CH), tile(lax.div(t, 2), QB)
            y[rows, cols] = dot(ov[rows, :], wo[:, cols], NN).astype(BF)

        return [((0, 1), None, y_body, 0, 20)]

    return Spec([o_rel, wo_rel], [sds(TOK, DM)], [], groups)


def last_fill(raw, w_dq, w_dkvt):
    def groups(f, bufs, outs, extra):
        rawv, wd, wk = bufs
        dx, = outs

        def dx_body(t):
            rows, cols = tile(lax.rem(t, 2), CH), tile(lax.div(t, 2), QB)
            g = dot(rawv[rows, :QL], wd[cols, :], NT) + dot(rawv[rows, QL:ALL], wk[:, cols], NN)
            dx[rows, cols] = g.astype(BF)

        return [((0, 1, 2), None, dx_body, 0, 20)]

    return Spec([raw, w_dq, w_dkvt], [sds(TOK, DM)], [], groups)


def zshift(v, d):
    return lax.ppermute(v, 'tp', [(i, (i + d) % NTP) for i in range(NTP)])


def zrel(v):
    return [v] + [zshift(v, d) for d in HOPS]


def norm_f32(raw_vals, gain_vec):
    inv_rms = lax.rsqrt(jnp.mean(raw_vals * raw_vals, axis=-1, keepdims=True) + EPS)
    return raw_vals * inv_rms * gain_vec


def solution(mesh):
    def per_device(hidden, grad_out, w_dq, g_q, w_dkv, g_kv, w_uq, w_uk, w_uv, w_o):
        rank = lax.axis_index('cp')
        z = lax.axis_index('tp')
        x2 = hidden.reshape(TOK, DM)
        dy2 = grad_out.reshape(TOK, DM)
        half = 16
        inv_freq = 1.0 / (THETA ** (jnp.arange(half, dtype=F32) * 2.0 / RD))
        idx = jnp.arange(QB, dtype=jnp.int32)
        positions = jnp.where(idx < HB, rank, NBLK - 1 - rank) * HB + idx % HB
        angles = positions.astype(F32)[:, None] * inv_freq[None, :]
        cos_tab, sin_tab = jnp.cos(angles), jnp.sin(angles)
        cos_t, sin_t = cos_tab.T, sin_tab.T
        gq = g_q.astype(F32)
        gkv = g_kv.astype(F32)

        kv_raw = dot(x2, w_dkv, NN).astype(BF)
        ckv_f32 = kv_raw[:, :QB].astype(F32)
        c_kv = norm_f32(ckv_f32, gkv).astype(BF)
        pe = kv_raw[:, QB:].astype(F32).reshape(4, QB, RD)
        pe1, pe2 = pe[..., :half], pe[..., half:]
        k_pe = jnp.concatenate([pe1 * cos_tab - pe2 * sin_tab, pe2 * cos_tab + pe1 * sin_tab], axis=-1).astype(BF)
        wo2 = w_o.reshape(HV, DM)
        w_qt = w_uq.transpose(1, 2, 0)
        w_q = jnp.concatenate([w_qt[:, :HD].reshape(NPAIR, HB, QL), w_qt[:, HD:].reshape(NPAIR, HD, QL), jnp.zeros((NPAIR, HD, QL), BF)], axis=1).reshape(QW, QL)
        kv, kpe, do, cq_raw, c_q, q = plane([c_kv, k_pe.transpose(1, 0, 2).reshape(QB, HB)], 0, False, True, filler=front_fill(x2, w_dq, g_q, dy2, wo2, w_q))
        q = q.reshape(4, QB, QW)
        do = do.reshape(4, QB, HV)
        kv = kv.reshape(NCP, 4, QB, QB)

        wo_rel = jnp.stack(zrel(lax.dynamic_slice_in_dim(wo2, rank * 80, 80, 0)))
        wo_rel, kv = lax.optimization_barrier((wo_rel, kv))
        wo_rel = lax.all_gather(wo_rel, 'cp', axis=1, tiled=True).reshape(DM, DM)

        wk = w_uk.transpose(1, 2, 0).reshape(HV, QB)
        wv = w_uv.transpose(1, 2, 0).reshape(HV, QB)

        n_split = 4
        nb = 4 // n_split
        runs = []
        for i in range(n_split):
            prev = [runs[-1][4], runs[-1][1], runs[-1][3]] if runs else []
            runs.append(attention(rank.reshape(1), q, do, wk, wv, cos_t, sin_t, kv, kpe, prev, i * nb, nb))
        o_rel = []
        for run in runs:
            parts = [run[0]]
            for d in HOPS:
                parts.append(zshift(run[0], d))
            o_rel.append(jnp.concatenate(parts, axis=2))
        o_rel = jnp.concatenate(o_rel, axis=0).reshape(TOK, DM)
        o = jnp.concatenate([run[0] for run in runs], axis=0).reshape(TOK, HV)
        dq = runs[-1][1].reshape(TOK, QW)
        dwkv = sum(run[2] for run in runs)

        dckv, dkpe, lat_q, dwo, dwq = plane([runs[-1][3].reshape(NCP, TOK, QB), runs[-1][4]], 1, True, False, filler=mid_fill(dq, w_q, o, dy2, c_q))
        dkpe = dkpe.reshape(QB, 4, RD).transpose(1, 0, 2)
        lat = jnp.concatenate([lat_q.reshape(4, QB, QL), dckv.reshape(4, QB, QB).astype(BF), dkpe.astype(BF), jnp.zeros((4, QB, DWW - ALL), BF)], axis=-1)
        cq_own = lax.dynamic_slice_in_dim(cq_raw, z * QB, QB, 0)
        ckv_own = lax.dynamic_slice_in_dim(kv_raw, z * QB, QB, 0)[:, :QB]
        dwq = dwq.reshape(NCP, KD, QL)
        dwkv = dwkv.reshape(NCP, KD, QB).astype(BF)
        dwo = dwo.reshape(NCP, 80, DM)
        raw, grad_g, dwq, dwkv, dwo, attn_out = plane([dwq, dwkv, dwo], 3, True, True, 1, [lat, cq_own, ckv_own, gq[None], gkv[None], cos_tab, sin_tab], y_fill(o_rel, wo_rel))
        raw_all = raw.reshape(TOK, DWW)

        x_slice = lax.dynamic_slice_in_dim(x2, z * HV, HV, 1)
        dwd = lax.dynamic_update_slice(dot(x_slice, raw_all, TN).astype(BF), grad_g.reshape(HB, NCP).astype(BF), (0, ALL)).reshape(NCP, 80, DWW)
        dwd, grad_hidden = plane([dwd], 2, True, True, NTP, filler=last_fill(raw.reshape(TOK, DWW), w_dq, w_dkv.T))
        grad_hidden = grad_hidden.reshape(4, QB, DM)
        attn_out = attn_out.reshape(4, QB, DM)
        dwd = dwd.reshape(DM, DWW)
        grad_g = jnp.sum(dwd.reshape(NTP, HV, DWW)[:, :HB, ALL:ALL + NCP].astype(F32), axis=0).reshape(TOK)
        dwq = dwq.reshape(NPAIR, QB, QL).astype(F32)
        grad_uq = jnp.concatenate([dwq[:, :HB].reshape(10, HD, QL), dwq[:, HB:HB + HD].reshape(10, RD, QL)], axis=1).transpose(2, 0, 1)
        dwkv = dwkv.reshape(NPAIR, QB, QB).astype(F32)
        grad_uk = dwkv[:, :HB].reshape(10, HD, QB).transpose(2, 0, 1)
        grad_uv = dwkv[:, HB:].reshape(10, HD, QB).transpose(2, 0, 1)
        return (attn_out, grad_hidden, dwd[:, :QL].astype(F32), grad_g[:QL], dwd[:, QL:ALL].astype(F32), grad_g[QL:], grad_uq, grad_uk, grad_uv, dwo.reshape(HV, DM).astype(F32).reshape(10, HD, DM))

    seq_spec = P(None, 'cp', None)
    full_spec = P()
    head_spec = P(None, 'tp', None)
    out_head_spec = P('tp', None, None)
    all_specs = (seq_spec, seq_spec, full_spec, full_spec, full_spec, full_spec, head_spec, head_spec, head_spec, out_head_spec)
    return jax.shard_map(per_device, mesh=mesh, in_specs=all_specs, out_specs=all_specs, check_vma=False)
```

```python
import functools
import math

import jax
import jax.numpy as jnp
from jax import lax
from jax.experimental import pallas as pl
from jax.experimental.pallas import tpu as pltpu
from jax.sharding import PartitionSpec as P


EPS = 1e-6
THETA = 10000.0
NEG_BIG = -1e30
BF = jnp.bfloat16
F32 = jnp.float32
NT = (((1,), (1,)), ((), ()))
TN = (((0,), (0,)), ((), ()))
NN = (((1,), (0,)), ((), ()))
HB, QB, CH, SEQ = 128, 256, 512, 2048
HD, KD, RD, QL = 64, 160, 32, 768
NBLK, NCP, NTP, NPAIR, NBAT = 16, 8, 4, 5, 4
TOK, DM, HV, QW, ALL, DWW = 1024, 2560, 640, 1280, 1056, 1152
RH = 16
HOPS = range(1, NTP)


def cost(flops):
    return pl.CostEstimate(flops=flops, bytes_accessed=TOK * TOK, transcendentals=0)


def dot(a, b, dims):
    return lax.dot_general(a, b, dims, preferred_element_type=F32)


def owner(blk):
    if blk < NCP:
        return blk, slice(0, HB)
    return NBLK - 1 - blk, slice(HB, QB)


def attn_kernel(b0, r_ref, q_ref, do_ref, wk_ref, wv_ref, cos_ref, sin_ref, *rest):
    kv_ref, kpe_ref = rest[:2]
    if b0 > 0:
        old_ref = rest[2]
    rest = rest[2 if b0 == 0 else 5:]
    o_ref, dq_ref, dw_ref, dkv_ref, dkpe_ref, ckv, ckvt, kcat, vv, s_scr, dp_scr, dk_acc, dv_acc, dckv, dkpe, qbd, dobd = rest
    b = pl.program_id(0)
    p = pl.program_id(1)
    n_pair = pl.num_programs(1)
    r = r_ref[0]
    scale = 96.0 ** -0.5
    c2 = scale * math.log2(math.e)

    @pl.when(p == 0)
    def _():
        for blk in range(NBLK):
            rows = slice(blk * HB, (blk + 1) * HB)
            dev, part = owner(blk)
            ckv[rows, :] = kv_ref[dev, 0, part, :]
            kcat[rows, HB:KD] = kpe_ref[dev, part, b0 * RD:(b0 + 1) * RD]
        for i in range(NBAT):
            ckvt[:, i * CH:(i + 1) * CH] = ckv[i * CH:(i + 1) * CH, :].T
        dckv[...] = jnp.zeros_like(dckv)
        dkpe[...] = jnp.zeros_like(dkpe)

    wkv = jnp.concatenate([wk_ref[...], wv_ref[...]], axis=0)
    for i in range(NBAT):
        rows = slice(i * CH, (i + 1) * CH)
        kv = dot(ckv[rows, :], wkv, NT).astype(BF)
        kcat[rows, 0:HB] = kv[:, 0:HB]
        vv[rows, :] = kv[:, HB:QB]

    cos_t = cos_ref[...]
    sin_t = sin_ref[...]
    lane = lax.broadcasted_iota(jnp.int32, (HB, HB), 1)
    zero = jnp.zeros((HB, HB), BF)
    qpt = q_ref[0, :, HB:QB].astype(F32).T
    roped = []
    for h in range(2):
        u1 = qpt[h * 32:h * 32 + 16, :]
        u2 = qpt[h * 32 + 16:h * 32 + 32, :]
        roped.append(u1 * cos_t - u2 * sin_t)
        roped.append(u2 * cos_t + u1 * sin_t)
    qpe = jnp.concatenate(roped + [jnp.zeros((HD, QB), F32)], axis=0).T.astype(BF)
    for s in range(2):
        rows = slice(s * HB, (s + 1) * HB)
        qn = q_ref[0, rows, 0:HB]
        gg = do_ref[0, rows, :]
        qbd[s, 0:HB, 0:HB] = jnp.where(lane < HD, qn, zero)
        qbd[s, HB:QB, 0:HB] = jnp.where(lane < HD, zero, qn)
        qbd[s, 0:HB, HB:KD] = qpe[rows, 0:32]
        qbd[s, HB:QB, HB:KD] = qpe[rows, 32:64]
        dobd[s, 0:HB, :] = jnp.where(lane < HD, gg, zero)
        dobd[s, HB:QB, :] = jnp.where(lane < HD, zero, gg)

    low = r < 4
    sel3 = jnp.where(low, 1, 0)
    chunks = [(1, 0), (1, 1), (1, 2), (sel3, jnp.where(low, 3, 0)), (0, jnp.where(low, 0, 1))]

    def keys(c):
        kc = chunks[c][1]
        if isinstance(kc, int):
            return slice(kc * CH, (kc + 1) * CH)
        return pl.ds(pl.multiple_of(kc * CH, CH), CH)

    diff = (lax.broadcasted_iota(jnp.int32, (CH, QB), 0)
            - lax.rem(lax.broadcasted_iota(jnp.int32, (CH, QB), 1), HB))
    maxes = []
    for c in range(5):
        sel, kc = chunks[c]
        s = dot(kcat[keys(c), :], qbd[sel], NT)
        if c >= 2:
            blk = jnp.where(sel == 1, 15 - r, r)
            s = jnp.where(diff <= blk * HB - kc * CH, s, NEG_BIG)
        s_scr[c] = s
        maxes.append(jnp.max(s, axis=0, keepdims=True))

    def join(vals, op, ident):
        ident = jnp.full_like(vals[3], ident)
        top = op(op(op(vals[0], vals[1]), vals[2]), jnp.where(low, vals[3], ident))
        bot = op(vals[4], jnp.where(low, ident, vals[3]))
        return [top, top, top, jnp.where(low, top, bot), bot]

    m = join(maxes, jnp.maximum, NEG_BIG)
    sums, dots = [], []
    for c in range(5):
        sel, kc = chunks[c]
        e = jnp.exp2((s_scr[c] - m[c]) * c2)
        s_scr[c] = e
        sums.append(jnp.sum(e, axis=0, keepdims=True))
        dp = dot(vv[keys(c), :], dobd[sel], NT)
        dp_scr[c] = dp
        dots.append(jnp.sum(e * dp, axis=0, keepdims=True))
    total = join(sums, jnp.add, 0.0)
    inv = [1.0 / t for t in total]
    dsum = join(dots, jnp.add, 0.0)
    delta = [d * i for d, i in zip(dsum, inv)]
    ots, dqts = [], []
    dk_acc[3 * CH:SEQ, :] = jnp.zeros((CH, KD), F32)
    dv_acc[3 * CH:SEQ, :] = jnp.zeros((CH, HB), F32)
    for c in range(5):
        sel, kc = chunks[c]
        pr = s_scr[c] * inv[c]
        pb = pr.astype(BF)
        ds = (pr * (dp_scr[c] - delta[c])).astype(BF)
        ots.append(dot(vv[keys(c), :], pb, TN))
        dqts.append(dot(kcat[keys(c), :], ds, TN))
        dv = dot(pb, dobd[sel], NN)
        dk = dot(ds, qbd[sel], NN)
        if c < 3:
            dk_acc[keys(c), :] = dk
            dv_acc[keys(c), :] = dv
        else:
            dk_acc[keys(c), :] += dk
            dv_acc[keys(c), :] += dv
    ot = join(ots, jnp.add, 0.0)
    dqt = join(dqts, jnp.add, 0.0)
    for s in range(2):
        rows = slice(s * HB, (s + 1) * HB)
        a = ot[0 if s == 1 else 4]
        o_ref[0, rows, :] = jnp.concatenate([a[0:HD, 0:HB], a[HD:HB, HB:QB]], axis=0).T.astype(BF)
        g = dqt[0 if s == 1 else 4] * scale
        dq_ref[0, rows, 0:HB] = jnp.concatenate([g[0:HD, 0:HB], g[HD:HB, HB:QB]], axis=0).T.astype(BF)
        pe = []
        for h in range(2):
            g1 = g[128:144, h * HB:(h + 1) * HB]
            g2 = g[144:160, h * HB:(h + 1) * HB]
            ct = cos_t[:, rows]
            st = sin_t[:, rows]
            pe.append(g1 * ct + g2 * st)
            pe.append(g2 * ct - g1 * st)
        dq_ref[0, rows, HB:QB] = jnp.concatenate(pe + [jnp.zeros((HD, HB), F32)], axis=0).T.astype(BF)

    dwt = jnp.zeros((QB, QB), F32)
    for i in range(NBAT):
        rows = slice(i * CH, (i + 1) * CH)
        dkv = jnp.concatenate([(dk_acc[rows, 0:HB] * scale).astype(BF), dv_acc[rows, :].astype(BF)], axis=1)
        dkpe[rows, :] += dk_acc[rows, HB:KD] * scale
        dckv[rows, :] += dot(dkv, wkv, NN)
        dwt = dwt + dot(ckvt[:, rows], dkv, NN)
    dwt = dwt.T

    @pl.when(b == 0)
    def _():
        dw_ref[p] = dwt

    @pl.when(b > 0)
    def _():
        dw_ref[p] += dwt

    @pl.when(p == n_pair - 1)
    def _():
        for blk in range(NBLK):
            rows = slice(blk * HB, (blk + 1) * HB)
            dev, part = owner(blk)
            dkv_ref[dev, 0, part, :] = dckv[rows, :].astype(BF)
            piece = dkpe[rows, :].astype(BF)
            if b0 > 0:
                dkpe_ref[dev, part, :] = old_ref[dev, part, :]
            dkpe_ref[dev, part, b0 * RD:(b0 + 1) * RD] = piece


def attention(rank, q, do, wk, wv, cos_t, sin_t, kv, kpe, prev, b0, nb):
    pair_blk = lambda w: pl.BlockSpec((1, QB, w), lambda b, p, *_: (b0 + b, 0, p))
    out_blk = lambda w: pl.BlockSpec((1, QB, w), lambda b, p, *_: (b, 0, p))
    w_blk = pl.BlockSpec((HB, QB), lambda b, p, *_: (p, 0))
    full = pl.BlockSpec((16, QB), lambda b, p, *_: (0, 0))
    kv_blk = pl.BlockSpec((NCP, 1, QB, QB), lambda b, p, *_: (0, b0 + b, 0, 0))
    dkv_blk = kv_blk
    pe_blk = pl.BlockSpec((NCP, QB, HB), lambda b, p, *_: (0, 0, 0))
    anyspec = [pe_blk] + [pl.BlockSpec(memory_space=pl.ANY)] * 2 if prev else []
    grid_spec = pltpu.PrefetchScalarGridSpec(
        num_scalar_prefetch=1,
        grid=(nb, NPAIR),
        in_specs=[pair_blk(QB), pair_blk(HB), w_blk, w_blk, full, full, kv_blk, pe_blk] + anyspec,
        out_specs=[out_blk(HB), pair_blk(QB), pl.BlockSpec((NPAIR, QB, QB), lambda b, p, *_: (0, 0, 0)), dkv_blk,
                   pe_blk],
        scratch_shapes=[
            pltpu.VMEM((SEQ, QB), BF), pltpu.VMEM((QB, SEQ), BF), pltpu.VMEM((SEQ, KD), BF), pltpu.VMEM((SEQ, HB), BF),
            pltpu.VMEM((5, CH, QB), F32), pltpu.VMEM((5, CH, QB), F32),
            pltpu.VMEM((SEQ, KD), F32), pltpu.VMEM((SEQ, HB), F32),
            pltpu.VMEM((SEQ, QB), F32), pltpu.VMEM((SEQ, RD), F32),
            pltpu.VMEM((2, QB, KD), BF), pltpu.VMEM((2, QB, HB), BF),
        ])
    return pl.pallas_call(
        functools.partial(attn_kernel, b0),
        grid_spec=grid_spec,
        out_shape=[jax.ShapeDtypeStruct((nb, QB, HV), BF), jax.ShapeDtypeStruct((NBAT, QB, QW), BF), jax.ShapeDtypeStruct((NPAIR, QB, QB), F32),
                   jax.ShapeDtypeStruct((NCP, 4, QB, QB), BF),
                   jax.ShapeDtypeStruct((NCP, QB, HB), BF)],
        compiler_params=pltpu.CompilerParams(vmem_limit_bytes=50 * TOK * TOK),
        cost_estimate=cost(nb * 20_000_000_000),
        input_output_aliases={10: 1, 11: 3} if prev else {},
        name="attn",
    )(rank, q, do, wk, wv, cos_t, sin_t, kv, kpe, *prev)


def norm_pull(grad, vals, gain):
    rr = lax.rsqrt(jnp.mean(vals * vals, axis=-1, keepdims=True) + EPS)
    h = grad * gain
    mix = jnp.mean(h * vals, axis=-1, keepdims=True) * (rr * rr * rr)
    return rr * h - vals * mix, jnp.sum(grad * (vals * rr), axis=0, keepdims=True)


class Filler:
    def __init__(self, filler, refs):
        n_in, n_out, n_extra = len(filler.args), len(filler.outs), len(filler.extra)
        src, self.outs, refs = refs[:n_in], refs[n_in:n_in + n_out], refs[n_in + n_out:]
        n_buf = len(filler.bufs)
        self.bufs, sems, extra = refs[:n_buf], refs[n_buf], refs[n_buf + 1:n_buf + 1 + n_extra]
        self.loads = [pltpu.make_async_copy(a, b, sems.at[i]) for i, (a, b) in enumerate(filler.place(src, self.bufs))]
        for c in self.loads:
            c.start()
        self.ready = [False] * n_in
        self.groups = [list(g) for g in filler.groups(self, self.bufs, self.outs, extra)]

    def need(self, which):
        for i in which:
            if not self.ready[i]:
                self.ready[i] = True
                self.loads[i].wait()

    def run(self, k):
        while k > 0 and self.groups:
            which, prep, body, lo, hi = self.groups[0]
            self.need(which)
            if prep is not None:
                prep()
            n = min(k, hi - lo)

            def step(t, carry):
                body(t)
                return carry

            lax.fori_loop(lo, lo + n, step, 0)
            k -= n
            if lo + n == hi:
                self.groups.pop(0)
            else:
                self.groups[0] = [which, None, body, lo + n, hi]


class NoFill:
    def run(self, k):
        return None


class Spec:
    def __init__(self, args, outs, extra, groups, bufs=(), place=zip):
        self.args, self.outs, self.extra, self.groups = args, outs, extra, groups
        self.bufs = bufs or [a.shape for a in args]
        self.place = place


def tile(t, n):
    return pl.ds(pl.multiple_of(t * n, n), n)


def plane_kernel(n_arr, reduce, gather, n_z, with_lat, filler, *refs):
    ins, refs = refs[:n_arr], refs[n_arr:]
    n_fill = len(filler.args) if filler else 0
    if with_lat:
        lats, refs = refs[:3], refs[3:]
        cq_ref, ckv_ref, gq_ref, gkv_ref, cos_ref, sin_ref = refs[:6]
        refs = refs[6:]
    fill_src, refs = refs[:n_fill], refs[n_fill:]
    if with_lat:
        (raw, gg), refs = refs[:2], refs[2:]
    outs, refs = refs[:n_arr], refs[n_arr:]
    fill_out, refs = (refs[:len(filler.outs)], refs[len(filler.outs):]) if filler else ((), refs)
    r = lax.axis_index('cp')
    z = lax.axis_index('tp')
    send, recv, scratch = refs[0], refs[1], refs[2:]
    pc, px, py = [{'cp': r ^ m} for m in (1, 2, 4)]
    barrier = pltpu.get_barrier_semaphore()
    targets = [pc, px, py] + [{'tp': lax.rem(z + d, NTP)} for d in range(1, NTP if with_lat else n_z)]
    for t in targets:
        pl.semaphore_signal(barrier, inc=1, device_id=t, device_id_type=pl.DeviceIdType.MESH)
    pl.semaphore_wait(barrier, len(targets))
    count = [0]
    started = []
    n_tail = (len(filler.bufs) + 1 + len(filler.extra)) if filler else 0
    fill = Filler(filler, list(fill_src) + list(fill_out) + list(scratch[len(scratch) - n_tail:])) if filler else NoFill()

    def copy(src, dst, target):
        k = count[0]
        count[0] += 1
        c = pltpu.make_async_remote_copy(src_ref=src, dst_ref=dst, send_sem=send.at[k], recv_sem=recv.at[k],
                                         device_id=target, device_id_type=pl.DeviceIdType.MESH)
        c.start()
        started.append(c)
        return c

    hop_base = count[0]
    if with_lat:
        count[0] += 2 * NTP

    def line(right, h):
        blk = raw.at[lax.rem(z + (NTP + 1 - h if right else NTP + h - 1), NTP)]
        k = hop_base + h + (0 if right else NTP)
        c = pltpu.make_async_remote_copy(src_ref=blk, dst_ref=blk, send_sem=send.at[k], recv_sem=recv.at[k],
                                         device_id={'tp': lax.rem(z + (1 if right else NTP - 1), NTP)}, device_id_type=pl.DeviceIdType.MESH)
        on = jnp.logical_and(z < NTP - 1, z >= h - 1) if right else jnp.logical_and(z > 0, z <= NTP - h)
        return c, on

    def hop(h):
        for right in (True, False):
            c, on = line(right, h)

            @pl.when(on)
            def _():
                if h > 1:
                    line(right, h - 1)[0].wait_recv()
                c.start()

    def hop_end():
        for right in (True, False):
            @pl.when(z == (NTP - 1 if right else 0))
            def _():
                for h in HOPS:
                    line(right, h)[0].wait_recv()

            for h in HOPS:
                c, on = line(right, h)
                pl.when(on)(c.wait_send)

    work = []
    for i in range(n_arr):
        w = {'in': ins[i], 'out': outs[i]}
        if reduce:
            w['rc'], w['sb'], w['rd'], w['rx'], w['ry'] = scratch[:5]
            scratch = scratch[5:]
            rows = w['rd'].shape[0]
        else:
            rows = ins[i].shape[0]
        w['g'] = outs[i]
        w['a'] = slice(0, (rows // 2 + RH - 1) // RH * RH)
        w['b'] = slice(w['a'].stop, rows)
        work.append(w)
    if with_lat:
        zrs = scratch[:3]
        z_in = [copy(a.at[lax.rem(z + d, NTP)], b.at[d - 1], {'tp': lax.rem(z + d, NTP)}) for d in HOPS for a, b in zip(lats, zrs)]
    if reduce:
        for w in work:
            w['c'] = [None] * 4
        for k in (3, 1, 2, 0):
            for w in work:
                w['c'][k] = copy(w['in'].at[r ^ (2 * k + 1)], w['rc'].at[k], pc)

        fill.run(2 if n_z > 1 else 8)

        def local(w, k):
            w['c'][k].wait_recv()
            return w['in'][r ^ (2 * k)].astype(F32) + w['rc'][k].astype(F32)

        for w in work:
            w['sb'][3] = local(w, 3).astype(BF)
            w['da'] = copy(w['sb'].at[3, w['a']], w['rd'].at[w['a']], px)
            w['db'] = copy(w['sb'].at[3, w['b']], w['rd'].at[w['b']], py)
        fill.run(NTP // n_z)
        for w in work:
            w['sb'][1] = local(w, 1).astype(BF)
            w['xa'] = copy(w['sb'].at[1, w['a']], w['rx'].at[w['a']], px)
            w['sb'][2] = local(w, 2).astype(BF)
            w['yb'] = copy(w['sb'].at[2, w['b']], w['ry'].at[w['b']], py)
        fill.run(4)
        for w in work:
            w['da'].wait_recv()
            w['sb'][2, w['a']] = (w['sb'][2, w['a']].astype(F32) + w['rd'][w['a']].astype(F32)).astype(BF)
            w['ya'] = copy(w['sb'].at[2, w['a']], w['ry'].at[w['a']], py)
            w['db'].wait_recv()
            w['sb'][1, w['b']] = (w['sb'][1, w['b']].astype(F32) + w['rd'][w['b']].astype(F32)).astype(BF)
            w['xb'] = copy(w['sb'].at[1, w['b']], w['rx'].at[w['b']], px)
        fill.run(6)
        for w in work:
            base = local(w, 0)
            for name in ('xa', 'yb', 'ya', 'xb'):
                w[name].wait_recv()
            total = base + w['rx'][...].astype(F32) + w['ry'][...].astype(F32)
            if gather:
                w['g'][z * NCP * (n_z > 1) + r] = total.astype(BF)
            else:
                w['out'][...] = total.astype(BF)
    elif gather:
        for w in work:
            w['g'][r] = w['in'][...]
    if gather:
        def fan(w, zz):
            own = w['g'].at[zz + r]
            return {'zz': zz, 'x': copy(own, own, px), 'y': copy(own, own, py), 'c': copy(own, own, pc)}

        flows = []
        z_copies = []
        for w in work:
            if n_z > 1:
                own = w['g'].at[z * NCP + r]
                z_copies.append([copy(own, own, {'tp': lax.rem(z + d, NTP)}) for d in range(1, n_z)])
            flows.append([fan(w, z * NCP if n_z > 1 else 0)])
        if with_lat:
            fill.run(10)
            for c in z_in:
                c.wait_recv()
            for i in range(NBAT):
                rows = slice(i * HD, (i + 1) * HD)
                own = []
                for a, b in zip(lats, zrs):
                    t = a[z, rows, :].astype(F32)
                    for d in range(NTP - 1):
                        t = t + b[d, rows, :].astype(F32)
                    own.append(t)
                g_cq, part_q = norm_pull(own[0], cq_ref[rows, :].astype(F32), gq_ref[...])
                g_ckv, part_kv = norm_pull(own[1], ckv_ref[rows, :].astype(F32), gkv_ref[...])
                p1, p2 = own[2][:, :RH], own[2][:, RH:RD]
                cc, ss = cos_ref[rows, :], sin_ref[rows, :]
                raw[z, rows, :] = jnp.concatenate([g_cq, g_ckv, p1 * cc + p2 * ss, p2 * cc - p1 * ss, jnp.zeros((HD, DWW - ALL), F32)], axis=1).astype(BF)
                part = jnp.concatenate([part_q, part_kv], axis=1)
                gg[...] = part if i == 0 else gg[...] + part
            hop(1)
        for d in range(n_z):
            fill.run(4)
            for i, w in enumerate(work):
                f = flows[i][d]
                gx, gy = w['g'].at[f['zz'] + (r ^ 2)], w['g'].at[f['zz'] + (r ^ 4)]
                f['x'].wait_recv()
                f['dy'] = copy(gx.at[w['b']], gx.at[w['b']], py)
                f['cx'] = copy(gx, gx, pc)
                f['y'].wait_recv()
                f['dx'] = copy(gy.at[w['a']], gy.at[w['a']], px)
                f['cy'] = copy(gy, gy, pc)
                if d + 1 < n_z:
                    z_copies[i][d].wait_recv()
                    flows[i].append(fan(w, lax.rem(z + NTP - (d + 1), NTP) * NCP))
        fill.run(3)
        if with_lat:
            hop(2)
        for d in range(n_z):
            for i, w in enumerate(work):
                f = flows[i][d]
                f['dy'].wait_recv()
                f['dx'].wait_recv()
                gd = w['g'].at[f['zz'] + (r ^ 6)]
                f['cd'] = copy(gd, gd, pc)
        fill.run(QB)
        if with_lat:
            hop(3)
        for d in range(n_z):
            for i, w in enumerate(work):
                f = flows[i][d]
                for name in ('c', 'cx', 'cy', 'cd'):
                    f[name].wait_recv()
        if with_lat:
            hop_end()
    fill.run(QB)
    for c in started:
        c.wait_send()


def plane(arrs, cid, reduce, gather, n_z=1, extra=(), filler=None):
    scratch, shapes = [], []
    n_copy = 0
    for v in arrs:
        n, m = v.shape[-2:]
        if reduce:
            scratch += [pltpu.VMEM((4, n, m), BF), pltpu.VMEM((4, n, m), BF)] + [pltpu.VMEM((n, m), BF)] * 3
            n_copy += 10
        if gather:
            shapes.append(jax.ShapeDtypeStruct((NCP * n_z, n, m), BF))
            n_copy += 8 * n_z + n_z - 1
        else:
            shapes.append(jax.ShapeDtypeStruct((n, m), BF))
    vmem = pl.BlockSpec(memory_space=pltpu.VMEM)
    if extra:
        shapes = [jax.ShapeDtypeStruct((NBAT, QB, DWW), BF), jax.ShapeDtypeStruct((1, TOK), F32)] + shapes
        scratch += [pltpu.VMEM((3,) + a.shape[1:], BF) for a in extra[:3]]
        n_copy += 18
    anyspec = []
    fill_args = ()
    if filler:
        fill_args = filler.args
        shapes += filler.outs
        anyspec = [pl.BlockSpec(memory_space=pl.ANY)] * len(filler.args)
        scratch += [pltpu.VMEM(shape, BF) for shape in filler.bufs] + [pltpu.SemaphoreType.DMA((len(filler.args),))] + filler.extra
    return pl.pallas_call(
        functools.partial(plane_kernel, len(arrs), reduce, gather, n_z, bool(extra), filler),
        out_shape=shapes,
        in_specs=[vmem] * (len(arrs) + len(extra)) + anyspec,
        out_specs=[vmem] * len(shapes),
        scratch_shapes=[pltpu.SemaphoreType.DMA((n_copy,)), pltpu.SemaphoreType.DMA((n_copy,))] + scratch,
        compiler_params=pltpu.CompilerParams(collective_id=cid, has_side_effects=True, vmem_limit_bytes=60 * TOK * TOK),
        cost_estimate=cost(30_000_000_000),
        name="plane",
    )(*arrs, *extra, *fill_args)


def sds(*shape):
    return jax.ShapeDtypeStruct(shape, BF)


def front_fill(x2, w_dq, gq, dy2, wo2, w_q):
    def groups(f, bufs, outs, extra):
        x, wd, dy, wo, wq, gain = bufs
        do, cq_raw, c_q, q = outs

        def do_body(t):
            do[tile(t, QB), :] = dot(dy[tile(t, QB), :], wo[...], NT).astype(BF)

        def q_body(t):
            u = dot(x[tile(t, QB), :], wd[...], NN).astype(BF)
            cq_raw[tile(t, QB), :] = u
            c = norm_f32(u.astype(F32), gain[...].astype(F32)).astype(BF)
            c_q[tile(t, QB), :] = c
            q[tile(t, QB), :] = dot(c, wq[...], NT).astype(BF)

        return [((2, 3), None, do_body, 0, 4), ((0, 1, 4, 5), None, q_body, 0, 4)]

    return Spec([x2, w_dq, dy2, wo2, w_q, gq[None]], [sds(TOK, HV), sds(TOK, QL), sds(TOK, QL), sds(TOK, QW)], [], groups)


def mid_fill(dq, w_q, o, dy2, c_q):
    def groups(f, bufs, outs, extra):
        dqv, wq, ov, dy, cq = bufs
        lat_q, dwo, dwq = outs
        ot, dqt = extra

        def lat_body(t):
            lat_q[tile(t, QB), :] = dot(dqv[tile(t, QB), :], wq[...], NN).astype(BF)

        def turn_o(t):
            ot[:, tile(t, QB)] = ov[tile(t, QB), :].T

        def dwo_body(t):
            dwo[:, tile(t, QB)] = dot(ot[...], dy[:, tile(t, QB)], NN).astype(BF)

        def turn_dq(t):
            dqt[:, tile(t, QB)] = dqv[tile(t, QB), :].T

        def dwq_body(t):
            dwq[:, tile(t, QB)] = dot(dqt[...], cq[:, tile(t, QB)], NN).astype(BF)

        return [((0, 1), None, lat_body, 0, 4), ((2,), None, turn_o, 0, 4), ((3,), None, dwo_body, 0, 10),
                ((), None, turn_dq, 0, 4), ((4,), None, dwq_body, 0, 3)]

    return Spec([dq, w_q, o, dy2, c_q], [sds(TOK, QL), sds(HV, DM), sds(QW, QL)], [pltpu.VMEM((HV, TOK), BF), pltpu.VMEM((QW, TOK), BF)], groups)


def y_fill(o_parts, wo_rel):
    def place(src, bufs):
        pairs = []
        for i in range(NBAT):
            for d in range(NTP):
                pairs.append((src[len(pairs)].at[0], bufs[0].at[i * QB:(i + 1) * QB, d * HV:(d + 1) * HV]))
        return pairs + [(src[len(pairs)], bufs[1])]

    def groups(f, bufs, outs, extra):
        ov, wo = bufs
        y, = outs

        def y_body(t):
            rows, cols = tile(lax.rem(t, 2), CH), tile(lax.div(t, 2), QB)
            y[rows, cols] = dot(ov[rows, :], wo[:, cols], NN).astype(BF)

        return [(range(len(o_parts) + 1), None, y_body, 0, 20)]

    return Spec(o_parts + [wo_rel], [sds(TOK, DM)], [], groups, [(TOK, DM), (DM, DM)], place)


def last_fill(raw, w_dq, w_dkvt):
    def groups(f, bufs, outs, extra):
        rawv, wd, wk = bufs
        dx, = outs

        def dx_body(t):
            rows, cols = tile(lax.rem(t, 2), CH), tile(lax.div(t, 2), QB)
            g = dot(rawv[rows, :QL], wd[cols, :], NT) + dot(rawv[rows, QL:ALL], wk[:, cols], NN)
            dx[rows, cols] = g.astype(BF)

        return [((0, 1, 2), None, dx_body, 0, 20)]

    return Spec([raw, w_dq, w_dkvt], [sds(TOK, DM)], [], groups)


def zshift(v, d):
    return lax.ppermute(v, 'tp', [(i, (i + d) % NTP) for i in range(NTP)])


def zrel(v):
    return [v] + [zshift(v, d) for d in HOPS]


def norm_f32(raw_vals, gain_vec):
    inv_rms = lax.rsqrt(jnp.mean(raw_vals * raw_vals, axis=-1, keepdims=True) + EPS)
    return raw_vals * inv_rms * gain_vec


def solution(mesh):
    def per_device(hidden, grad_out, w_dq, g_q, w_dkv, g_kv, w_uq, w_uk, w_uv, w_o):
        rank = lax.axis_index('cp')
        z = lax.axis_index('tp')
        x2 = hidden.reshape(TOK, DM)
        dy2 = grad_out.reshape(TOK, DM)
        half = RH
        inv_freq = 1.0 / (THETA ** (jnp.arange(half, dtype=F32) * 2.0 / RD))
        idx = jnp.arange(QB, dtype=jnp.int32)
        positions = jnp.where(idx < HB, rank, NBLK - 1 - rank) * HB + idx % HB
        angles = positions.astype(F32)[:, None] * inv_freq[None, :]
        cos_tab, sin_tab = jnp.cos(angles), jnp.sin(angles)
        cos_t, sin_t = cos_tab.T, sin_tab.T
        gq = g_q.astype(F32)
        gkv = g_kv.astype(F32)

        kv_raw = dot(x2, w_dkv, NN).astype(BF)
        ckv_f32 = kv_raw[:, :QB].astype(F32)
        c_kv = norm_f32(ckv_f32, gkv).astype(BF)
        pe = kv_raw[:, QB:].astype(F32).reshape(NBAT, QB, RD)
        pe1, pe2 = pe[..., :half], pe[..., half:]
        k_pe = jnp.concatenate([pe1 * cos_tab - pe2 * sin_tab, pe2 * cos_tab + pe1 * sin_tab], axis=-1).astype(BF)
        wo2 = w_o.reshape(HV, DM)
        w_qt = w_uq.transpose(1, 2, 0)
        w_q = jnp.concatenate([w_qt[:, :HD].reshape(NPAIR, HB, QL), w_qt[:, HD:].reshape(NPAIR, HD, QL), jnp.zeros((NPAIR, HD, QL), BF)], axis=1).reshape(QW, QL)
        kv, kpe, do, cq_raw, c_q, q = plane([c_kv, k_pe.transpose(1, 0, 2).reshape(QB, HB)], 0, False, True, filler=front_fill(x2, w_dq, g_q, dy2, wo2, w_q))
        q = q.reshape(NBAT, QB, QW)
        do = do.reshape(NBAT, QB, HV)
        kv = kv.reshape(NCP, 4, QB, QB)

        wo_rel = jnp.stack(zrel(lax.dynamic_slice_in_dim(wo2, rank * 80, 80, 0)))
        wo_rel, kv = lax.optimization_barrier((wo_rel, kv))
        wo_rel = lax.all_gather(wo_rel, 'cp', axis=1, tiled=True).reshape(DM, DM)

        wk = w_uk.transpose(1, 2, 0).reshape(HV, QB)
        wv = w_uv.transpose(1, 2, 0).reshape(HV, QB)

        n_split = NBAT
        nb = NBAT // n_split
        runs = []
        for i in range(n_split):
            prev = [runs[-1][4], runs[-1][1], runs[-1][3]] if runs else []
            runs.append(attention(rank.reshape(1), q, do, wk, wv, cos_t, sin_t, kv, kpe, prev, i * nb, nb))
        o_parts = []
        for run in runs:
            o_parts.append(run[0])
            for d in HOPS:
                o_parts.append(zshift(run[0], d))
        o = jnp.concatenate([run[0] for run in runs], axis=0).reshape(TOK, HV)
        dq = runs[-1][1].reshape(TOK, QW)
        dwkv = sum(run[2] for run in runs)

        dckv, dkpe, lat_q, dwo, dwq = plane([runs[-1][3].reshape(NCP, TOK, QB), runs[-1][4]], 1, True, False, filler=mid_fill(dq, w_q, o, dy2, c_q))
        dkpe = dkpe.reshape(QB, 4, RD).transpose(1, 0, 2)
        lats = [lat_q.reshape(NBAT, QB, QL), dckv.reshape(NBAT, QB, QB), jnp.pad(dkpe, ((0, 0), (0, 0), (0, HB - RD)))]
        cq_own = lax.dynamic_slice_in_dim(cq_raw, z * QB, QB, 0)
        ckv_own = lax.dynamic_slice_in_dim(kv_raw, z * QB, QB, 0)[:, :QB]
        dwq = dwq.reshape(NCP, KD, QL)
        dwkv = dwkv.reshape(NCP, KD, QB).astype(BF)
        dwo = dwo.reshape(NCP, 80, DM)
        raw, grad_g, dwq, dwkv, dwo, attn_out = plane([dwq, dwkv, dwo], 3, True, True, 1, lats + [cq_own, ckv_own, gq[None], gkv[None], cos_tab, sin_tab], y_fill(o_parts, wo_rel))
        raw_all = raw.reshape(TOK, DWW)

        x_slice = lax.dynamic_slice_in_dim(x2, z * HV, HV, 1)
        dwd = lax.dynamic_update_slice(dot(x_slice, raw_all, TN).astype(BF), grad_g.reshape(HB, NCP).astype(BF), (0, ALL)).reshape(NCP, 80, DWW)
        dwd, grad_hidden = plane([dwd], 2, True, True, NTP, filler=last_fill(raw.reshape(TOK, DWW), w_dq, w_dkv.T))
        grad_hidden = grad_hidden.reshape(NBAT, QB, DM)
        attn_out = attn_out.reshape(NBAT, QB, DM)
        dwd = dwd.reshape(DM, DWW)
        grad_g = jnp.sum(dwd.reshape(NTP, HV, DWW)[:, :HB, ALL:ALL + NCP].astype(F32), axis=0).reshape(TOK)
        dwq = dwq.reshape(NPAIR, QB, QL).astype(F32)
        grad_uq = jnp.concatenate([dwq[:, :HB].reshape(10, HD, QL), dwq[:, HB:HB + HD].reshape(10, RD, QL)], axis=1).transpose(2, 0, 1)
        dwkv = dwkv.reshape(NPAIR, QB, QB).astype(F32)
        grad_uk = dwkv[:, :HB].reshape(10, HD, QB).transpose(2, 0, 1)
        grad_uv = dwkv[:, HB:].reshape(10, HD, QB).transpose(2, 0, 1)
        return (attn_out, grad_hidden, dwd[:, :QL].astype(F32), grad_g[:QL], dwd[:, QL:ALL].astype(F32), grad_g[QL:], grad_uq, grad_uk, grad_uv, dwo.reshape(HV, DM).astype(F32).reshape(10, HD, DM))

    seq_spec = P(None, 'cp', None)
    full_spec = P()
    head_spec = P(None, 'tp', None)
    out_head_spec = P('tp', None, None)
    all_specs = (seq_spec, seq_spec, full_spec, full_spec, full_spec, full_spec, head_spec, head_spec, head_spec, out_head_spec)
    return jax.shard_map(per_device, mesh=mesh, in_specs=all_specs, out_specs=all_specs, check_vma=False)
```
